128 devices in a mesh: fsdp: 2 (over core), ep: 64 (over z, y, x).
Axes of the slice: x: 4, y: 4, z: 4, core: 2. Of those that a mesh axis runs over, the one named last changes fastest.
Arguments:
- x_tok: bfloat16 [262144, 512], P(('fsdp', 'ep'))
- dy_tok: bfloat16 [262144, 512], P(('fsdp', 'ep'))
- expert_ids: int32 [262144, 2], P(('fsdp', 'ep'))
- route_w: float32 [262144, 2], P(('fsdp', 'ep'))
- w_gate: bfloat16 [128, 512, 512], P('ep', 'fsdp')
- w_up: bfloat16 [128, 512, 512], P('ep', 'fsdp')
- w_down: bfloat16 [128, 512, 512], P('ep', None, 'fsdp')
Outputs:
- output 1: bfloat16 [262144, 512], P(('fsdp', 'ep'))
- output 2: float32 [262144, 2], P(('fsdp', 'ep'))
- output 3: float32 [128, 512, 512], P('ep', 'fsdp')
- output 4: float32 [128, 512, 512], P('ep', 'fsdp')
- output 5: float32 [128, 512, 512], P('ep', None, 'fsdp')
All inputs are finite; a program needn't handle non-finite values.
Results may differ from the reference program's by a relative error of at most 0.001.
Values are sent between devices in bfloat16 or wider.
A program may use at most 1 GiB of HBM per device.

```python
import jax
import jax.numpy as jnp
from jax import lax

D_MODEL = 512
D_FF = 512
EXPERTS = 128
TOP_K = 2
TOK_DEV = 2048
DEVICES = 128
CAPACITY = 96

TOKENS = DEVICES * TOK_DEV
SLOTS = EXPERTS * CAPACITY
HOT_COUNT = max(1, TOP_K // 2)


def draw_routing(root_key):
    key_hot, key_score = jax.random.split(root_key)
    hot_rank = jax.random.permutation(key_hot, EXPERTS)
    bias = jnp.where(hot_rank < HOT_COUNT, 768, 0).astype(jnp.int32)
    expert_col = jnp.arange(EXPERTS, dtype=jnp.int32)

    def one_device(dev_key):
        noise = jax.random.randint(dev_key, (TOK_DEV, EXPERTS), 0, 1024, dtype=jnp.int32)
        score = (noise + bias[None, :]) * EXPERTS + expert_col[None, :]
        return lax.top_k(score, TOP_K)[1]

    chosen = lax.map(one_device, jax.random.split(key_score, DEVICES))
    return chosen.reshape(TOKENS, TOP_K).astype(jnp.int32)


def setup_inputs(seed: int = 0) -> dict:
    key_list = jax.random.split(jax.random.key(seed), 7)
    x_tok = jax.random.normal(key_list[0], (TOKENS, D_MODEL), jnp.float32)
    dy_tok = jax.random.normal(key_list[1], (TOKENS, D_MODEL), jnp.float32)
    expert_ids = draw_routing(key_list[2])
    route_w = jax.random.uniform(key_list[3], (TOKENS, TOP_K), jnp.float32, 0.1, 1.0)
    w_gate = jax.random.normal(key_list[4], (EXPERTS, D_MODEL, D_FF), jnp.float32) * D_MODEL ** -0.5
    w_up = jax.random.normal(key_list[5], (EXPERTS, D_MODEL, D_FF), jnp.float32) * D_MODEL ** -0.5
    w_down = jax.random.normal(key_list[6], (EXPERTS, D_FF, D_MODEL), jnp.float32) * D_FF ** -0.5
    return {
        "x_tok": x_tok.astype(jnp.bfloat16),
        "dy_tok": dy_tok.astype(jnp.bfloat16),
        "expert_ids": expert_ids,
        "route_w": route_w,
        "w_gate": w_gate.astype(jnp.bfloat16),
        "w_up": w_up.astype(jnp.bfloat16),
        "w_down": w_down.astype(jnp.bfloat16),
    }


def slot_positions(ids_dev):
    onehot = (ids_dev[:, None] == jnp.arange(EXPERTS, dtype=jnp.int32)[None, :]).astype(jnp.int32)
    before = jnp.cumsum(onehot, axis=0) - onehot
    position = jnp.sum(before * onehot, axis=1)
    return jnp.where(position < CAPACITY, ids_dev * CAPACITY + position, SLOTS)


def swiglu_grads(pre_gate, pre_up, grad_hidden):
    sigma = jax.nn.sigmoid(pre_gate)
    grad_gate = grad_hidden * pre_up * sigma * (1.0 + pre_gate * (1.0 - sigma))
    grad_up = grad_hidden * pre_gate * sigma
    return grad_gate.astype(jnp.bfloat16), grad_up.astype(jnp.bfloat16)


def reference(x_tok, dy_tok, expert_ids, route_w, w_gate, w_up, w_down):
    dest_slot = lax.map(slot_positions, expert_ids.reshape(DEVICES, TOK_DEV * TOP_K))
    pair_ids = jnp.arange(TOKENS * TOP_K, dtype=jnp.int32).reshape(DEVICES, TOK_DEV * TOP_K)
    dev_rows = jnp.broadcast_to(jnp.arange(DEVICES, dtype=jnp.int32)[:, None], dest_slot.shape)
    slot_src = jnp.full((DEVICES, SLOTS + 1), TOKENS * TOP_K, jnp.int32)
    slot_src = slot_src.at[dev_rows, dest_slot].set(pair_ids)[:, :SLOTS]
    per_expert = slot_src.reshape(DEVICES, EXPERTS, CAPACITY).transpose(1, 0, 2).reshape(EXPERTS, DEVICES * CAPACITY)
    route_flat = route_w.reshape(-1)

    def expert_step(carry, step_in):
        dx_acc, dr_acc = carry
        pair_src, w_gate_e, w_up_e, w_down_e = step_in
        tok_rows = pair_src // TOP_K
        x_rows = jnp.take(x_tok, tok_rows, axis=0, mode="fill", fill_value=0)
        dy_rows = jnp.take(dy_tok, tok_rows, axis=0, mode="fill", fill_value=0)
        gate_rows = jnp.take(route_flat, pair_src, axis=0, mode="fill", fill_value=0)
        pre_gate = jnp.dot(x_rows, w_gate_e, preferred_element_type=jnp.float32)
        pre_up = jnp.dot(x_rows, w_up_e, preferred_element_type=jnp.float32)
        hidden = (jax.nn.silu(pre_gate) * pre_up).astype(jnp.bfloat16)
        y_rows = jnp.dot(hidden, w_down_e, preferred_element_type=jnp.float32)
        dy_wide = dy_rows.astype(jnp.float32)
        scaled_dy = (gate_rows[:, None] * dy_wide).astype(jnp.bfloat16)
        dr_rows = jnp.sum(dy_wide * y_rows, axis=1)
        grad_hidden = jnp.dot(scaled_dy, w_down_e.T, preferred_element_type=jnp.float32)
        grad_gate, grad_up = swiglu_grads(pre_gate, pre_up, grad_hidden)
        dx_rows = (jnp.dot(grad_gate, w_gate_e.T, preferred_element_type=jnp.float32)
                   + jnp.dot(grad_up, w_up_e.T, preferred_element_type=jnp.float32)).astype(jnp.bfloat16)
        dw_gate = jnp.dot(x_rows.T, grad_gate, preferred_element_type=jnp.float32)
        dw_up = jnp.dot(x_rows.T, grad_up, preferred_element_type=jnp.float32)
        dw_down = jnp.dot(hidden.T, scaled_dy, preferred_element_type=jnp.float32)
        dx_acc = dx_acc.at[tok_rows].add(dx_rows.astype(jnp.float32), mode="drop")
        dr_acc = dr_acc.at[pair_src].set(dr_rows, mode="drop")
        return (dx_acc, dr_acc), (dw_gate, dw_up, dw_down)

    init = (jnp.zeros((TOKENS, D_MODEL), jnp.float32), jnp.zeros((TOKENS * TOP_K,), jnp.float32))
    (dx_acc, dr_acc), (grad_w_gate, grad_w_up, grad_w_down) = lax.scan(
        expert_step, init, (per_expert, w_gate, w_up, w_down))
    grad_x = dx_acc.astype(jnp.bfloat16)
    route_w_grad = dr_acc.reshape(TOKENS, TOP_K)
    return (grad_x, route_w_grad, grad_w_gate, grad_w_up, grad_w_down)
```

```python
import functools

import jax
import jax.numpy as jnp
from jax import lax
from jax.experimental import pallas as pl
from jax.experimental.pallas import tpu as pltpu
from jax.sharding import PartitionSpec as P

CAP_FACTOR = 3
LANES = 128
ROWS_G = 256
FAR = 1 << 20
f32, bf16, i32 = jnp.float32, jnp.bfloat16, jnp.int32


def capacity_of(tok_dev, top_k, experts):
    return max(8, ((CAP_FACTOR * tok_dev * top_k // experts + 7) // 8) * 8)


def iota(shape, dim):
    return lax.broadcasted_iota(i32, shape, dim)


def nn(a, b):
    return jnp.dot(a, b, preferred_element_type=f32)


def nt(a, b):
    return lax.dot_general(a, b, (((1,), (1,)), ((), ())), preferred_element_type=f32)


def tn(a, b):
    return lax.dot_general(a, b, (((0,), (0,)), ((), ())), preferred_element_type=f32)


def split3(v):
    hi = v.astype(bf16)
    rest = v - hi.astype(f32)
    mid = rest.astype(bf16)
    lo = (rest - mid.astype(f32)).astype(bf16)
    return hi, mid, lo


def add3(v, n):
    return v[:, :n] + v[:, n:2 * n] + v[:, 2 * n:]


def exact(a, b):
    return jnp.dot(a, b, preferred_element_type=f32, precision=lax.Precision.HIGHEST)


def route_kernel(capacity, rows, span, ids_ref, rw_ref, q_ref, msg_ref):
    experts, chunk = LANES, 256
    tokens = ids_ref.shape[1]
    n_dest = msg_ref.shape[0]
    before = (iota((chunk, chunk), 0) < iota((chunk, chunk), 1)).astype(bf16)
    expert_id = iota((experts, chunk), 0)
    slot_id = iota((span, chunk), 0)
    half_id = iota((n_dest, chunk), 0) * 2
    seen = jnp.zeros((experts, 1), f32)
    gates = [jnp.zeros((3 * n_dest, span), f32) for _ in range(2)]
    for c in range(tokens // chunk):
        at = slice(c * chunk, (c + 1) * chunk)
        id_rows = [ids_ref[j:j + 1, at] for j in range(2)]
        hits = [expert_id == row for row in id_rows]
        member = jnp.where(hits[0] | hits[1], 1.0, 0.0)
        earlier = nn(member.astype(bf16), before) + seen
        seen = seen + jnp.sum(member, axis=1, keepdims=True)
        for j in range(2):
            place = jnp.sum(jnp.where(hits[j], earlier, 0.0), axis=0, keepdims=True).astype(i32)
            slot = jnp.where(id_rows[j] % 2 == 0, place, rows - 1 - place)
            slot = jnp.where(place < capacity, slot, FAR)
            q_ref[j:j + 1, at] = jnp.where(place < capacity, (id_rows[j] // 2) * rows + slot, FAR)
            slot_hot = jnp.where(slot_id == slot, 1.0, 0.0).astype(bf16)
            weight = rw_ref[j:j + 1, at]
            for par in range(2):
                mine = jnp.where(half_id + par == id_rows[j], weight, 0.0)
                gates[par] = gates[par] + nt(jnp.concatenate(split3(mine), axis=0), slot_hot)
    kept = jnp.broadcast_to(jnp.minimum(seen, float(capacity)), (experts, LANES)).astype(bf16)
    owner = (iota((n_dest, experts), 1) // 2 == iota((n_dest, experts), 0)).astype(bf16)
    over = jnp.where(nn(owner, kept) > float(rows), 1.0, 0.0)
    for par in range(2):
        g = gates[par]
        msg_ref[:, par * span:(par + 1) * span] = g[:n_dest] + g[n_dest:2 * n_dest] + g[2 * n_dest:]
    msg_ref[:, 2 * span:] = jnp.broadcast_to(jnp.max(over, axis=0, keepdims=True), (n_dest, LANES))


def pack_kernel(q_ref, x_ref, dy_ref, out_ref):
    d = x_ref.shape[1]
    row = iota((ROWS_G, q_ref.shape[1]), 0) + pl.program_id(0) * ROWS_G
    pick = jnp.where((q_ref[0:1, :] == row) | (q_ref[1:2, :] == row), 1.0, 0.0).astype(bf16)
    out_ref[:, :d] = nn(pick, x_ref[...]).astype(bf16)
    out_ref[:, d:] = nn(pick, dy_ref[...]).astype(bf16)


def expert_kernel(depth, span, xdy_ref, rec_ref, wg_ref, wu_ref, wd_ref,
                  dx_ref, dr_ref, dwg_ref, dwu_ref, dwd_ref, w2_ref):
    step = pl.program_id(0)
    group, rows, width = xdy_ref.shape
    n_src = rec_ref.shape[0]
    d = width // 2
    half = wg_ref.shape[2]
    m = group * depth

    @pl.when(step == 0)
    def _():
        for ref in (dr_ref, dwg_ref, dwu_ref, dwd_ref):
            ref[...] = jnp.zeros_like(ref)
        for k in range(2):
            for i in range(2):
                w2_ref[k, :, i * half:(i + 1) * half] = wd_ref[i, k]

    local = iota((m, n_src), 0) // depth + step * group
    src_hot = jnp.where(local == iota((m, n_src), 1), 1.0, 0.0).astype(bf16)
    within = iota((m, span), 0) % depth
    outs = []
    for k in range(2):
        first = 0 if k == 0 else rows - depth
        slot_hot = iota((m, span), 1) == within + first
        gate_parts = jnp.concatenate(split3(rec_ref[:, k * span:(k + 1) * span]), axis=1)
        weight = jnp.sum(jnp.where(slot_hot, add3(nn(src_hot, gate_parts), span), 0.0), axis=1, keepdims=True)
        x = xdy_ref[:, first:first + depth, :d].reshape(m, d)
        dy = xdy_ref[:, first:first + depth, d:].reshape(m, d).astype(f32)
        w1 = wg_ref[:, k].reshape(d, wg_ref.shape[3])
        w3 = wu_ref[:, k].reshape(d, wu_ref.shape[3])
        w2 = w2_ref[k]
        h1 = nn(x, w1)
        h3 = nn(x, w3)
        s = jax.nn.sigmoid(h1)
        hidden = (h1 * s * h3).astype(bf16)
        dr = jnp.sum(dy * nn(hidden, w2), axis=1, keepdims=True)
        g = (weight * dy).astype(bf16)
        da = nt(g, w2)
        dh1 = (da * h3 * s * (1.0 + h1 * (1.0 - s))).astype(bf16)
        dh3 = (da * h1 * s).astype(bf16)
        outs.append((nt(dh1, w1) + nt(dh3, w3)).reshape(group, depth, d))
        dwg_ref[k] += tn(x, dh1)
        dwu_ref[k] += tn(x, dh3)
        dwd_ref[k] += tn(hidden, g)
        parts = jnp.concatenate(split3(jnp.where(slot_hot, dr, 0.0)), axis=1)
        dr_ref[:, k * span:(k + 1) * span] += add3(tn(src_hot, parts), span)
    low = rows - depth
    dx_ref[:, :low] = outs[0][:, :low].astype(bf16)
    if depth > low:
        dx_ref[:, low:depth] = (outs[0][:, low:] + outs[1][:, :depth - low]).astype(bf16)
    dx_ref[:, depth:] = outs[1][:, depth - low:].astype(bf16)


def dr_kernel(rows, span, ids_ref, q_ref, back_ref, out_ref):
    n_src = back_ref.shape[0]
    tokens = ids_ref.shape[1]
    table = back_ref[...].T
    chunk = 512
    for c in range(tokens // chunk):
        at = slice(c * chunk, (c + 1) * chunk)
        for j in range(2):
            ids = ids_ref[j:j + 1, at]
            q = q_ref[j:j + 1, at]
            owner = jnp.where(iota((n_src, chunk), 0) == ids // 2, 1.0, 0.0)
            column = exact(table, owner)
            want = jnp.where(q < FAR, (ids % 2) * span + q - (ids // 2) * rows, FAR)
            out_ref[j:j + 1, at] = jnp.sum(
                jnp.where(iota((2 * span, chunk), 0) == want, column, 0.0), axis=0, keepdims=True)


def combine_kernel(q_ref, back_ref, out_ref):
    rows, depth = q_ref.shape[0], 512
    q0, q1 = q_ref[:, 0:1], q_ref[:, 1:2]

    def body(i, acc):
        at = i * depth
        column = iota((rows, depth), 1) + at
        pick = jnp.where((q0 == column) | (q1 == column), 1.0, 0.0).astype(bf16)
        return acc + nn(pick, back_ref[pl.ds(pl.multiple_of(at, depth), depth), :])

    steps = back_ref.shape[0] // depth
    out_ref[...] = lax.fori_loop(0, steps, body, jnp.zeros(out_ref.shape, f32)).astype(bf16)


def vmem():
    return pl.BlockSpec(memory_space=pltpu.VMEM)


def whole(shape):
    return pl.BlockSpec(shape, lambda i: (0,) * len(shape))


PARAMS = pltpu.CompilerParams(vmem_limit_bytes=60 * 1024 * 1024)


def exchange(v):
    return lax.all_to_all(v, "ep", 0, 0, tiled=True)


class Plan:
    def __init__(self, rows, depth, group, capacity, n_ep):
        self.rows, self.depth, self.group, self.capacity, self.n_ep = rows, depth, group, capacity, n_ep
        self.span = -(-rows // LANES) * LANES

    def forward(self, x_tok, dy_tok, ids_t, rw_t, weights):
        tok_dev, d = x_tok.shape
        n_ep, rows, span = self.n_ep, self.rows, self.span
        q_t, msg = pl.pallas_call(
            functools.partial(route_kernel, self.capacity, rows, span),
            out_shape=(jax.ShapeDtypeStruct((2, tok_dev), i32), jax.ShapeDtypeStruct((n_ep, 2 * span + LANES), f32)),
            in_specs=[vmem(), vmem()], out_specs=(vmem(),) * 2, compiler_params=PARAMS, name="route",
        )(ids_t, rw_t)
        rec = exchange(msg)
        packed = pl.pallas_call(
            pack_kernel,
            out_shape=jax.ShapeDtypeStruct((n_ep * rows, 2 * d), bf16),
            grid=(n_ep * rows // ROWS_G,),
            in_specs=[whole((2, tok_dev)), whole((tok_dev, d)), whole((tok_dev, d))],
            out_specs=pl.BlockSpec((ROWS_G, 2 * d), lambda i: (i, 0)),
            compiler_params=PARAMS, name="pack",
        )(q_t, x_tok, dy_tok)
        xdy = exchange(packed.reshape(n_ep, rows, 2 * d))
        dx, dr, dwg, dwu, dwd = self.experts(xdy, rec, weights)
        dx_back = exchange(dx).reshape(n_ep * rows, d)
        dr_back = exchange(dr)
        dr_t = pl.pallas_call(
            functools.partial(dr_kernel, rows, span),
            out_shape=jax.ShapeDtypeStruct((2, tok_dev), f32),
            in_specs=[vmem()] * 3, out_specs=vmem(), compiler_params=PARAMS, name="route_grad",
        )(ids_t, q_t, dr_back)
        return rec[:, 2 * span:], q_t, dx_back, dr_t, (dwg, dwu, dwd)

    def experts(self, xdy, rec, weights):
        n_ep, rows, width = xdy.shape
        d, group, span = width // 2, self.group, self.span
        wg, wu, wd = weights
        ff = wg.shape[3]
        return pl.pallas_call(
            functools.partial(expert_kernel, self.depth, span),
            out_shape=(jax.ShapeDtypeStruct((n_ep, rows, d), bf16),
                       jax.ShapeDtypeStruct((n_ep, 2 * span), f32),
                       jax.ShapeDtypeStruct((2, d, ff), f32),
                       jax.ShapeDtypeStruct((2, d, ff), f32),
                       jax.ShapeDtypeStruct((2, ff, d), f32)),
            grid=(n_ep // group,),
            in_specs=[pl.BlockSpec((group, rows, width), lambda i: (i, 0, 0)),
                      whole(rec.shape), whole(wg.shape), whole(wu.shape), whole(wd.shape)],
            out_specs=(pl.BlockSpec((group, rows, d), lambda i: (i, 0, 0)),
                       whole((n_ep, 2 * span)), whole((2, d, ff)), whole((2, d, ff)), whole((2, ff, d))),
            scratch_shapes=[pltpu.VMEM((2, ff, d), bf16)],
            compiler_params=PARAMS, name="experts",
        )(xdy, rec, wg, wu, wd)

    def combine(self, q_t, dx_back):
        tok_dev, (slots, d), tile = q_t.shape[1], dx_back.shape, 256
        return pl.pallas_call(
            combine_kernel,
            out_shape=jax.ShapeDtypeStruct((tok_dev, d), bf16),
            grid=(tok_dev // tile,),
            in_specs=[pl.BlockSpec((tile, 2), lambda i: (i, 0)), whole((slots, d))],
            out_specs=pl.BlockSpec((tile, d), lambda i: (i, 0)),
            compiler_params=PARAMS, name="combine",
        )(q_t.T, dx_back)


def solution(mesh):
    n_ep = mesh.shape["ep"]
    tok_spec = P(("fsdp", "ep"), None)
    spec_in = P("ep", "fsdp", None)
    spec_out = P("ep", None, "fsdp")

    def per_device(x_tok, dy_tok, expert_ids, route_w, w_gate, w_up, w_down):
        tok_dev, top_k = expert_ids.shape
        capacity = capacity_of(tok_dev, top_k, w_gate.shape[0] * n_ep)
        part = lax.axis_index("fsdp")
        swap = [(0, 1), (1, 0)]
        weights = [lax.all_gather(w, "fsdp", axis=0) for w in (w_gate, w_up, w_down)]
        inputs = (x_tok, dy_tok, expert_ids.T, route_w.T, weights)

        def shard_halves(dws):
            out = []
            for dw, axis in zip(dws, (1, 1, 2)):
                size = dw.shape[axis] // 2
                keep = lax.dynamic_slice_in_dim(dw, part * size, size, axis)
                give = lax.dynamic_slice_in_dim(dw, (1 - part) * size, size, axis)
                out.append(keep + lax.ppermute(give, "fsdp", swap))
            return out

        quick = Plan(128, capacity, 4, capacity, n_ep)
        safe = Plan(2 * capacity, capacity, 4, capacity, n_ep)
        flags, q_t, dx_back, dr_t, dws = quick.forward(*inputs)
        bad = jnp.max(flags).reshape(1, 1)
        bad = jnp.maximum(bad, lax.ppermute(bad, "fsdp", swap))

        def fits():
            return (quick.combine(q_t, dx_back), dr_t.T, *shard_halves(dws))

        def general():
            _, q_all, dx_all, dr_all, dw_all = safe.forward(*inputs)
            return (safe.combine(q_all, dx_all), dr_all.T, *shard_halves(dw_all))

        return lax.cond(bad[0, 0] == 0.0, fits, general)

    return jax.shard_map(
        per_device, mesh=mesh,
        in_specs=(tok_spec, tok_spec, tok_spec, tok_spec, spec_in, spec_in, spec_out),
        out_specs=(tok_spec, tok_spec, spec_in, spec_in, spec_out),
        check_vma=False)
```

```python
import functools

import jax
import jax.numpy as jnp
from jax import lax
from jax.experimental import pallas as pl
from jax.experimental.pallas import tpu as pltpu
from jax.sharding import PartitionSpec as P

CAP_FACTOR = 3
LANES = 128
FAR = 1 << 20
TAIL = 8
MESH = pl.DeviceIdType.MESH
f32, bf16, i32 = jnp.float32, jnp.bfloat16, jnp.int32


def capacity_of(tok_dev, top_k, experts):
    return max(8, ((CAP_FACTOR * tok_dev * top_k // experts + 7) // 8) * 8)


def iota(shape, dim):
    return lax.broadcasted_iota(i32, shape, dim)


def nn(a, b):
    return jnp.dot(a, b, preferred_element_type=f32)


def nt(a, b):
    return lax.dot_general(a, b, (((1,), (1,)), ((), ())), preferred_element_type=f32)


def tn(a, b):
    return lax.dot_general(a, b, (((0,), (0,)), ((), ())), preferred_element_type=f32)


def split3(v):
    hi = v.astype(bf16)
    rest = v - hi.astype(f32)
    mid = rest.astype(bf16)
    lo = (rest - mid.astype(f32)).astype(bf16)
    return hi, mid, lo


def add3(v, n):
    return v[:, :n] + v[:, n:2 * n] + v[:, 2 * n:]


def route_kernel(capacity, rows, depth, span, local_top, ids_ref, rw_ref, q_ref, pos_ref, msg_ref, top_ref, topw_ref):
    experts, chunk = LANES, 256
    tokens = ids_ref.shape[1]
    n_dest = msg_ref.shape[0]
    pitch = rows + TAIL
    before = (iota((chunk, chunk), 0) < iota((chunk, chunk), 1)).astype(bf16)
    expert_id = iota((experts, chunk), 0)
    slot_id = iota((span, chunk), 0)
    half_id = iota((n_dest, chunk), 0) * 2
    seen = jnp.zeros((experts, 1), f32)
    for c in range(tokens // chunk):
        at = slice(c * chunk, (c + 1) * chunk)
        hits = [expert_id == ids_ref[j:j + 1, at] for j in range(2)]
        member = jnp.where(hits[0] | hits[1], 1.0, 0.0)
        earlier = nn(member.astype(bf16), before) + seen
        seen = seen + jnp.sum(member, axis=1, keepdims=True)
        for j in range(2):
            pos_ref[j:j + 1, at] = jnp.sum(jnp.where(hits[j], earlier, 0.0), axis=0, keepdims=True).astype(i32)
    expert_col = iota((experts, 1), 0).astype(f32)
    kept = jnp.minimum(seen, float(capacity))
    if local_top:
        most = jnp.max(seen, axis=0, keepdims=True)
        top = jnp.min(jnp.where(seen == most, expert_col, float(experts)), axis=0, keepdims=True)
        kept = jnp.where(expert_col == top, 0.0, kept)
    else:
        top = jnp.full((1, 1), -1.0, f32)
    top_i = top.astype(i32)
    gates = [jnp.zeros((3 * n_dest, span), f32) for _ in range(2)]
    top_gates = jnp.zeros((24, LANES), f32)
    for c in range(tokens // chunk):
        at = slice(c * chunk, (c + 1) * chunk)
        for j in range(2):
            ids = ids_ref[j:j + 1, at]
            place = pos_ref[j:j + 1, at]
            weight = rw_ref[j:j + 1, at]
            keep = place < capacity
            slot = jnp.where(ids % 2 == 0, place, rows - 1 - place)
            q = (ids // 2) * pitch + slot
            if local_top:
                is_top = ids == top_i
                q = jnp.where(is_top, n_dest * pitch + place, q)
                slot = jnp.where(is_top, FAR, slot)
                top_hot = jnp.where((iota((LANES, chunk), 0) == place) & keep & is_top, 1.0, 0.0).astype(bf16)
                top_parts = [jnp.broadcast_to(p, (8, chunk)) for p in split3(weight)]
                top_gates = top_gates + nt(jnp.concatenate(top_parts, axis=0), top_hot)
            q_ref[j:j + 1, at] = jnp.where(keep, q, FAR)
            slot_hot = jnp.where(slot_id == jnp.where(keep, slot, FAR), 1.0, 0.0).astype(bf16)
            for par in range(2):
                mine = jnp.where(half_id + par == ids, weight, 0.0)
                gates[par] = gates[par] + nt(jnp.concatenate(split3(mine), axis=0), slot_hot)
    kept_wide = jnp.broadcast_to(kept, (experts, LANES)).astype(bf16)
    owner = (iota((n_dest, experts), 1) // 2 == iota((n_dest, experts), 0)).astype(bf16)
    over = jnp.max(jnp.where(nn(owner, kept_wide) > float(rows), 1.0, 0.0), axis=0, keepdims=True)
    over = jnp.maximum(over, jnp.max(jnp.where(kept > float(depth), 1.0, 0.0), axis=0, keepdims=True))
    for par in range(2):
        g = gates[par]
        msg_ref[:, par * span:(par + 1) * span] = g[:n_dest] + g[n_dest:2 * n_dest] + g[2 * n_dest:]
    note = jnp.where(iota((1, LANES), 1) == 1, top, over)
    msg_ref[:, 2 * span:] = jnp.broadcast_to(note, (n_dest, LANES))
    top_ref[...] = jnp.broadcast_to(top_i, (8, LANES))
    topw_ref[...] = top_gates[:8] + top_gates[8:16] + top_gates[16:]


def pack_kernel(group, rows, first, q_ref, x_ref, dy_ref, out_ref):
    d = x_ref.shape[1]
    count, tokens = group * rows, q_ref.shape[1]
    row = iota((count, tokens), 0)
    slot = row + (row // rows + pl.program_id(0) * group) * TAIL + pl.program_id(0) * count + first
    pick = jnp.where((q_ref[0:1, :] == slot) | (q_ref[1:2, :] == slot), 1.0, 0.0).astype(bf16)
    out_ref[:, :d] = nn(pick, x_ref[...]).astype(bf16)
    out_ref[:, d:] = nn(pick, dy_ref[...]).astype(bf16)


def swiglu_rows(x, dy, weight, w1, w3, w2):
    h1 = nn(x, w1)
    h3 = nn(x, w3)
    s = jax.nn.sigmoid(h1)
    hidden = (h1 * s * h3).astype(bf16)
    dr = jnp.sum(dy * nn(hidden, w2), axis=1, keepdims=True)
    g = (weight * dy).astype(bf16)
    da = nt(g, w2)
    dh1 = (da * h3 * s * (1.0 + h1 * (1.0 - s))).astype(bf16)
    dh3 = (da * h1 * s).astype(bf16)
    return hidden, g, dh1, dh3, nt(dh1, w1) + nt(dh3, w3), dr


def expert_kernel(depth, span, xdy_ref, rec_ref, wg_ref, wu_ref, wd_ref,
                  dx_ref, dwg_ref, dwu_ref, dwd_ref, w2_ref):
    step = pl.program_id(0)
    group, rows, width = xdy_ref.shape
    n_src = rec_ref.shape[0]
    d = width // 2
    half = wg_ref.shape[2]
    m = group * depth

    @pl.when(step == 0)
    def _():
        for ref in (dwg_ref, dwu_ref, dwd_ref):
            ref[...] = jnp.zeros_like(ref)
        for k in range(2):
            for i in range(2):
                w2_ref[k, :, i * half:(i + 1) * half] = wd_ref[i, k]

    local = iota((m, n_src), 0) // depth
    src_hot = jnp.where(local + step * group == iota((m, n_src), 1), 1.0, 0.0).astype(bf16)
    row_hot = jnp.where(iota((m, LANES), 0) // depth == iota((m, LANES), 1), 1.0, 0.0).astype(bf16)
    within = iota((m, span), 0) % depth
    outs, dr_slots = [], jnp.zeros((LANES, span), f32)
    for k in range(2):
        first = 0 if k == 0 else rows - depth
        slot_hot = iota((m, span), 1) == within + first
        gate_parts = jnp.concatenate(split3(rec_ref[:, k * span:(k + 1) * span]), axis=1)
        weight = jnp.sum(jnp.where(slot_hot, add3(nn(src_hot, gate_parts), span), 0.0), axis=1, keepdims=True)
        x = xdy_ref[:, first:first + depth, :d].reshape(m, d)
        dy = xdy_ref[:, first:first + depth, d:].reshape(m, d).astype(f32)
        w1 = wg_ref[:, k].reshape(d, wg_ref.shape[3])
        w3 = wu_ref[:, k].reshape(d, wu_ref.shape[3])
        hidden, g, dh1, dh3, dx, dr = swiglu_rows(x, dy, weight, w1, w3, w2_ref[k])
        outs.append(dx.reshape(group, depth, d))
        dwg_ref[k] += tn(x, dh1)
        dwu_ref[k] += tn(x, dh3)
        dwd_ref[k] += tn(hidden, g)
        parts = jnp.concatenate(split3(jnp.where(slot_hot & (weight > 0.0), dr, 0.0)), axis=1)
        dr_slots = dr_slots + add3(tn(row_hot, parts), span)
    low = rows - depth
    dx_ref[:, :low] = outs[0][:, :low].astype(bf16)
    if depth > low:
        dx_ref[:, low:depth] = (outs[0][:, low:] + outs[1][:, :depth - low]).astype(bf16)
    dx_ref[:, depth:rows] = outs[1][:, depth - low:].astype(bf16)
    parts = split3(dr_slots)
    for i in range(group):
        dx_ref[i, rows:, :] = jnp.zeros((TAIL, d), bf16)
        for n in range(3):
            dx_ref[i, rows + n:rows + n + 1, :span] = parts[n][i:i + 1, :]


def top_kernel(wm_ref, rows_ref, gate_ref, dx_ref, dr_ref, grad_ref,
               wbuf, wr0, wr1, wr2, wfull, gfull, gbuf, gpeer, gr0, gr1, gr2, ssem, rsem):
    me, part = lax.axis_index("ep"), lax.axis_index("fsdp")
    strides = (1, 4, 16)
    coord = [me % 4, (me // 4) % 4, me // 16]
    n_mat, total = wbuf.shape[0], wbuf.shape[1]
    levels = len(strides)

    def peer(axis, delta):
        return me + ((coord[axis] + delta) % 4 - coord[axis]) * strides[axis]

    barrier = pltpu.get_barrier_semaphore()
    for axis in range(3):
        for delta in (1, 2, 3):
            pl.semaphore_signal(barrier, inc=1, device_id={"ep": peer(axis, delta)}, device_id_type=MESH)
    pl.semaphore_signal(barrier, inc=1, device_id={"fsdp": 1 - part}, device_id_type=MESH)
    pl.semaphore_wait(barrier, 10)

    def at(base, size):
        return pl.ds(pl.multiple_of(base, 16), size)

    def all_reduce(which, buf, recvs, put):
        base = [0] * n_mat
        sizes, starts = [], []
        for level in range(levels):
            size = total // 4 ** (level + 1)
            copies = []
            for c in range(n_mat):
                axis = (c + level) % 3
                for delta in (1, 2, 3):
                    to = (coord[axis] + delta) % 4
                    copies.append(pltpu.make_async_remote_copy(
                        src_ref=buf.at[c, at(base[c] + to * size, size)],
                        dst_ref=recvs[level].at[c, 3 - delta],
                        send_sem=ssem.at[which, 0, level, c, delta - 1], recv_sem=rsem.at[which, 0, level, c, 3 - delta],
                        device_id={"ep": peer(axis, delta)}, device_id_type=MESH))
            for copy in copies:
                copy.start()
            for copy in copies:
                copy.wait()
            starts.append(list(base))
            sizes.append(size)
            for c in range(n_mat):
                base[c] = base[c] + coord[(c + level) % 3] * size
                mine = at(base[c], size)
                got = [recvs[level][c, i].astype(f32) for i in range(3)]
                buf[c, mine] = (buf[c, mine].astype(f32) + got[0] + got[1] + got[2]).astype(buf.dtype)
        for c in range(n_mat):
            put(c, at(base[c], sizes[-1]))[...] = buf[c, at(base[c], sizes[-1])]
        for level in reversed(range(levels)):
            copies = []
            for c in range(n_mat):
                axis = (c + level) % 3
                mine = at(starts[level][c] + coord[axis] * sizes[level], sizes[level])
                for delta in (1, 2, 3):
                    copies.append(pltpu.make_async_remote_copy(
                        src_ref=put(c, mine), dst_ref=put(c, mine),
                        send_sem=ssem.at[which, 1, level, c, delta - 1], recv_sem=rsem.at[which, 1, level, c, 3 - delta],
                        device_id={"ep": peer(axis, delta)}, device_id_type=MESH))
            for copy in copies:
                copy.start()
            for copy in copies:
                copy.wait()

    wbuf[...] = wm_ref[...]
    all_reduce(0, wbuf, (wr0, wr1, wr2), lambda c, s: wfull.at[part, c, s])
    swap = pltpu.make_async_remote_copy(
        src_ref=wfull.at[part], dst_ref=wfull.at[part], send_sem=ssem.at[0, 2, 0, 0, 0], recv_sem=rsem.at[0, 2, 0, 0, 0],
        device_id={"fsdp": 1 - part}, device_id_type=MESH)
    swap.start()
    swap.wait()

    d = dx_ref.shape[1]
    half = d // 2
    wide = d // LANES
    mats = []
    for i in range(2):
        mats.append(jnp.concatenate([jnp.concatenate(
            [wfull[f, i, b * half:(b + 1) * half, :] for b in range(wide)], axis=1) for f in range(2)], axis=0))
    w2 = jnp.concatenate([wfull[f, 2, b * d:(b + 1) * d, :] for f in range(2) for b in range(wide // 2)], axis=1)
    n = rows_ref.shape[0]
    x = rows_ref[:, :d]
    dy = rows_ref[:, d:].astype(f32)
    eye = iota((n, n), 0) == iota((n, n), 1)
    weight = jnp.sum(jnp.where(eye, gate_ref[0:1, :], 0.0), axis=1, keepdims=True)
    hidden, g, dh1, dh3, dx, dr = swiglu_rows(x, dy, weight, mats[0], mats[1], w2)
    dx_ref[...] = dx.astype(bf16)
    dr_ref[...] = jnp.broadcast_to(dr, dr_ref.shape)
    for i, dh in enumerate((dh1, dh3)):
        dw = tn(x, dh)
        for f in range(2):
            for b in range(wide):
                gfull[f, i, b * half:(b + 1) * half, :] = dw[f * half:(f + 1) * half, b * LANES:(b + 1) * LANES]
    dw = tn(hidden, g)
    for f in range(2):
        for b in range(wide // 2):
            lane = f * half + b * LANES
            gfull[f, 2, b * d:(b + 1) * d, :] = dw[:, lane:lane + LANES]

    swap = pltpu.make_async_remote_copy(
        src_ref=gfull.at[1 - part], dst_ref=gpeer, send_sem=ssem.at[1, 2, 0, 0, 0], recv_sem=rsem.at[1, 2, 0, 0, 0],
        device_id={"fsdp": 1 - part}, device_id_type=MESH)
    swap.start()
    swap.wait()
    gbuf[...] = gfull[part] + gpeer[...]
    all_reduce(1, gbuf, (gr0, gr1, gr2), lambda c, s: grad_ref.at[c, s])


def dr_kernel(rows, span, ids_ref, q_ref, pos_ref, back_ref, top_dr_ref, out_ref):
    n_src = back_ref.shape[0]
    tokens = ids_ref.shape[1]
    pitch = rows + TAIL
    chunk = 512
    tables = [back_ref[:, n, :span].T for n in range(3)]
    for c in range(tokens // chunk):
        at = slice(c * chunk, (c + 1) * chunk)
        for j in range(2):
            block = ids_ref[j:j + 1, at] // 2
            q = q_ref[j:j + 1, at]
            owner = jnp.where(iota((n_src, chunk), 0) == block, 1.0, 0.0).astype(bf16)
            column = nn(tables[0], owner) + nn(tables[1], owner) + nn(tables[2], owner)
            far = q >= n_src * pitch
            want = jnp.where(far, FAR, q - block * pitch)
            picked = jnp.sum(jnp.where(iota((span, chunk), 0) == want, column, 0.0), axis=0, keepdims=True)
            if top_dr_ref is not None:
                want = jnp.where(far, q - n_src * pitch, FAR)
                picked = picked + jnp.sum(
                    jnp.where(iota((LANES, chunk), 0) == want, top_dr_ref[:, 0:1], 0.0), axis=0, keepdims=True)
            out_ref[j:j + 1, at] = picked


def combine_kernel(q_ref, back_ref, *rest):
    top_ref, out_ref = rest if len(rest) == 2 else (None, rest[0])
    rows, slots = q_ref.shape[0], back_ref.shape[0]
    q0, q1 = q_ref[:, 0:1], q_ref[:, 1:2]
    acc = jnp.zeros(out_ref.shape, f32)
    for at in range(0, slots, 512):
        depth = min(512, slots - at)
        column = iota((rows, depth), 1) + at
        pick = jnp.where((q0 == column) | (q1 == column), 1.0, 0.0).astype(bf16)
        acc = acc + nn(pick, back_ref[at:at + depth, :])
    if top_ref is not None:
        column = iota((rows, LANES), 1) + slots
        pick = jnp.where((q0 == column) | (q1 == column), 1.0, 0.0).astype(bf16)
        acc = acc + nn(pick, top_ref[...])
    out_ref[...] = acc.astype(bf16)


def vmem():
    return pl.BlockSpec(memory_space=pltpu.VMEM)


def whole(shape):
    return pl.BlockSpec(shape, lambda i: (0,) * len(shape))


PARAMS = pltpu.CompilerParams(vmem_limit_bytes=60 * 1024 * 1024)


def exchange(v):
    return lax.all_to_all(v, "ep", 0, 0, tiled=True)


def top_serve(w_mine, rows, gate, d):
    n_mat, total = 3, w_mine.shape[1]
    scratch = []
    for dtype in (bf16, f32):
        recvs = [pltpu.VMEM((n_mat, 3, total // 4 ** (i + 1), LANES), dtype) for i in range(3)]
        if dtype == bf16:
            scratch += [pltpu.VMEM((n_mat, total, LANES), dtype), *recvs, pltpu.VMEM((2, n_mat, total, LANES), dtype)]
        else:
            scratch += [pltpu.VMEM((2, n_mat, total, LANES), dtype), pltpu.VMEM((n_mat, total, LANES), dtype),
                        pltpu.VMEM((n_mat, total, LANES), dtype), *recvs]
    scratch += [pltpu.SemaphoreType.DMA((2, 3, 3, n_mat, 3)), pltpu.SemaphoreType.DMA((2, 3, 3, n_mat, 3))]
    return pl.pallas_call(
        top_kernel,
        out_shape=(jax.ShapeDtypeStruct((rows.shape[0], d), bf16),
                   jax.ShapeDtypeStruct((rows.shape[0], LANES), f32),
                   jax.ShapeDtypeStruct((n_mat, total, LANES), f32)),
        in_specs=[vmem()] * 3, out_specs=(vmem(),) * 3, scratch_shapes=scratch,
        compiler_params=pltpu.CompilerParams(
            vmem_limit_bytes=48 * 1024 * 1024, collective_id=0, has_side_effects=True),
        cost_estimate=pl.CostEstimate(flops=40_000_000_000, bytes_accessed=8_000_000, transcendentals=0),
        name="top",
    )(w_mine, rows, gate)


class Plan:
    def __init__(self, rows, depth, pack_group, group, capacity, n_ep, local_top):
        self.rows, self.depth, self.pack_group, self.group = rows, depth, pack_group, group
        self.capacity, self.n_ep, self.local_top = capacity, n_ep, local_top
        self.span = -(-rows // LANES) * LANES

    def pack(self, q_t, x_tok, dy_tok, group, rows, steps, first):
        tok_dev, d = x_tok.shape
        return pl.pallas_call(
            functools.partial(pack_kernel, group, rows, first),
            out_shape=jax.ShapeDtypeStruct((steps * group * rows, 2 * d), bf16),
            grid=(steps,),
            in_specs=[whole((2, tok_dev)), whole((tok_dev, d)), whole((tok_dev, d))],
            out_specs=pl.BlockSpec((group * rows, 2 * d), lambda i: (i, 0)),
            compiler_params=PARAMS, name="pack",
        )(q_t, x_tok, dy_tok)

    def forward(self, me, x_tok, dy_tok, ids_t, rw_t, weights, own):
        tok_dev, d = x_tok.shape
        n_ep, rows, span = self.n_ep, self.rows, self.span
        q_t, pos_t, msg, top, top_gate = pl.pallas_call(
            functools.partial(route_kernel, self.capacity, rows, self.depth, span, self.local_top),
            out_shape=(jax.ShapeDtypeStruct((2, tok_dev), i32), jax.ShapeDtypeStruct((2, tok_dev), i32),
                       jax.ShapeDtypeStruct((n_ep, 2 * span + LANES), f32),
                       jax.ShapeDtypeStruct((8, LANES), i32), jax.ShapeDtypeStruct((8, LANES), f32)),
            in_specs=[vmem(), vmem()], out_specs=(vmem(),) * 5, compiler_params=PARAMS, name="route",
        )(ids_t, rw_t)
        rec = exchange(msg)
        packed = self.pack(q_t, x_tok, dy_tok, self.pack_group, rows, n_ep // self.pack_group, 0)
        top_out = None
        if self.local_top:
            top_rows = self.pack(q_t, x_tok, dy_tok, 1, LANES, 1, n_ep * (rows + TAIL))
            top_id = top[0, 0]
            mine = top_id // 2 == me
            flat = []
            for w in own:
                one = lax.dynamic_index_in_dim(w, top_id % 2, 0, keepdims=False)
                one = jnp.where(mine, one, jnp.zeros_like(one))
                flat.append(one.reshape(one.shape[0], -1, LANES).transpose(1, 0, 2).reshape(-1, LANES))
            packed, top_rows = lax.optimization_barrier((packed, top_rows))
            top_out = (top_id, *top_serve(jnp.stack(flat), top_rows, top_gate, d))
        xdy = exchange(packed.reshape(n_ep, rows, 2 * d))
        dx, dwg, dwu, dwd = self.experts(xdy, rec, weights)
        back = exchange(dx)
        return rec[:, 2 * span:], q_t, back, top_out, (dwg, dwu, dwd)

    def experts(self, xdy, rec, weights):
        n_ep, rows, width = xdy.shape
        d, group, span = width // 2, self.group, self.span
        wg, wu, wd = weights
        ff = wg.shape[3]
        return pl.pallas_call(
            functools.partial(expert_kernel, self.depth, span),
            out_shape=(jax.ShapeDtypeStruct((n_ep, rows + TAIL, d), bf16),
                       jax.ShapeDtypeStruct((2, d, ff), f32),
                       jax.ShapeDtypeStruct((2, d, ff), f32),
                       jax.ShapeDtypeStruct((2, ff, d), f32)),
            grid=(n_ep // group,),
            in_specs=[pl.BlockSpec((group, rows, width), lambda i: (i, 0, 0)),
                      whole(rec.shape), whole(wg.shape), whole(wu.shape), whole(wd.shape)],
            out_specs=(pl.BlockSpec((group, rows + TAIL, d), lambda i: (i, 0, 0)),
                       whole((2, d, ff)), whole((2, d, ff)), whole((2, ff, d))),
            scratch_shapes=[pltpu.VMEM((2, ff, d), bf16)],
            compiler_params=PARAMS, name="experts",
        )(xdy, rec, wg, wu, wd)

    def finish(self, ids_t, q_t, back, top_out):
        tok_dev, (n_ep, pitch, d), tile = q_t.shape[1], back.shape, 256
        tail = back[:, self.rows:, :]
        dr_args = [ids_t, q_t, q_t, tail] + ([top_out[2]] if top_out else [])
        kernel = functools.partial(dr_kernel, self.rows, self.span)
        if not top_out:
            inner = kernel
            kernel = lambda a, b, c, e, out: inner(a, b, c, e, None, out)
        dr_t = pl.pallas_call(
            kernel, out_shape=jax.ShapeDtypeStruct((2, tok_dev), f32),
            in_specs=[vmem()] * len(dr_args), out_specs=vmem(), compiler_params=PARAMS, name="route_grad",
        )(*dr_args)
        slots = n_ep * pitch
        args = [q_t.T, back.reshape(slots, d)] + ([top_out[1]] if top_out else [])
        grad_x = pl.pallas_call(
            combine_kernel,
            out_shape=jax.ShapeDtypeStruct((tok_dev, d), bf16),
            grid=(tok_dev // tile,),
            in_specs=[pl.BlockSpec((tile, 2), lambda i: (i, 0))] + [whole(v.shape) for v in args[1:]],
            out_specs=pl.BlockSpec((tile, d), lambda i: (i, 0)),
            compiler_params=PARAMS, name="combine",
        )(*args)
        return grad_x, dr_t.T


def solution(mesh):
    n_ep = mesh.shape["ep"]
    tok_spec = P(("fsdp", "ep"), None)
    spec_in = P("ep", "fsdp", None)
    spec_out = P("ep", None, "fsdp")

    def per_device(x_tok, dy_tok, expert_ids, route_w, w_gate, w_up, w_down):
        tok_dev, top_k = expert_ids.shape
        capacity = capacity_of(tok_dev, top_k, w_gate.shape[0] * n_ep)
        me, part = lax.axis_index("ep").astype(i32), lax.axis_index("fsdp")
        swap = [(0, 1), (1, 0)]
        own = (w_gate, w_up, w_down)
        weights = [lax.all_gather(w, "fsdp", axis=0) for w in own]
        ids_t = expert_ids.T
        inputs = (me, x_tok, dy_tok, ids_t, route_w.T, weights, own)

        def shard_halves(dws):
            out = []
            for dw, axis in zip(dws, (1, 1, 2)):
                size = dw.shape[axis] // 2
                keep = lax.dynamic_slice_in_dim(dw, part * size, size, axis)
                give = lax.dynamic_slice_in_dim(dw, (1 - part) * size, size, axis)
                out.append(keep + lax.ppermute(give, "fsdp", swap))
            return out

        quick = Plan(72, 48, 4, 8, capacity, n_ep, True)
        safe = Plan(2 * capacity, capacity, 2, 4, capacity, n_ep, False)
        notes, q_t, back, top_out, dws = quick.forward(*inputs)
        halves = shard_halves(dws)
        top_id = top_out[0]
        agree = jnp.all(notes[:, 1] == top_id.astype(f32)) & jnp.all(notes[:, 0] == 0.0)
        note = jnp.where(agree, top_id.astype(f32), -1.0).reshape(1, 1)
        other = lax.ppermute(note, "fsdp", swap)
        good = agree & (other == note)[0, 0]

        def fits():
            grads = []
            for i, half in enumerate(halves):
                rows = half.shape[1]
                extra = top_out[3][i].reshape(-1, rows, LANES).transpose(1, 0, 2).reshape(1, *half.shape[1:])
                pick = (jnp.arange(2) + 2 * me == top_id)[:, None, None]
                grads.append(half + jnp.where(pick, extra, 0.0))
            return (*quick.finish(ids_t, q_t, back, top_out), *grads)

        def general():
            _, q_all, back_all, _, dw_all = safe.forward(*inputs)
            return (*safe.finish(ids_t, q_all, back_all, None), *shard_halves(dw_all))

        return lax.cond(good, fits, general)

    return jax.shard_map(
        per_device, mesh=mesh,
        in_specs=(tok_spec, tok_spec, tok_spec, tok_spec, spec_in, spec_in, spec_out),
        out_specs=(tok_spec, tok_spec, spec_in, spec_in, spec_out),
        check_vma=False)
```

```python
import functools

import jax
import jax.numpy as jnp
from jax import lax
from jax.experimental import pallas as pl
from jax.experimental.pallas import tpu as pltpu
from jax.sharding import PartitionSpec as P

CAP_FACTOR = 3
LANES = 128
FAR = 1 << 20
TAIL = 8
MESH = pl.DeviceIdType.MESH
f32, bf16, i32 = jnp.float32, jnp.bfloat16, jnp.int32


def capacity_of(tok_dev, top_k, experts):
    return max(8, ((CAP_FACTOR * tok_dev * top_k // experts + 7) // 8) * 8)


def iota(shape, dim):
    return lax.broadcasted_iota(i32, shape, dim)


def nn(a, b):
    return jnp.dot(a, b, preferred_element_type=f32)


def nt(a, b):
    return lax.dot_general(a, b, (((1,), (1,)), ((), ())), preferred_element_type=f32)


def tn(a, b):
    return lax.dot_general(a, b, (((0,), (0,)), ((), ())), preferred_element_type=f32)


def split3(v):
    hi = v.astype(bf16)
    rest = v - hi.astype(f32)
    mid = rest.astype(bf16)
    lo = (rest - mid.astype(f32)).astype(bf16)
    return hi, mid, lo


def hot(mask):
    return jnp.where(mask, 1.0, 0.0).astype(bf16)


def only(mask, v):
    return jnp.where(mask, v, jnp.zeros_like(v))


def down(v):
    return jnp.sum(v, axis=0, keepdims=True)


def across(v):
    return jnp.sum(v, axis=1, keepdims=True)


def add3(v, n):
    return v[:, :n] + v[:, n:2 * n] + v[:, 2 * n:]


SIDE = 4
STRIDES = (1, SIDE, SIDE * SIDE)


def coords(me):
    return [me % SIDE, (me // SIDE) % SIDE, me // (SIDE * SIDE)]


def peer_at(me, r, sign):
    o = (r * 23) % SIDE ** 3
    out = 0
    for here, off, stride in zip(coords(me), coords(o), STRIDES):
        out = out + ((here + sign * off + SIDE) % SIDE) * stride
    return out


def meet_all(me, part):
    barrier = pltpu.get_barrier_semaphore()
    n = SIDE ** 3

    @pl.loop(1, n)
    def _(r):
        pl.semaphore_signal(barrier, inc=1, device_id={"ep": peer_at(me, r, 1)}, device_id_type=MESH)

    pl.semaphore_signal(barrier, inc=1, device_id={"fsdp": 1 - part}, device_id_type=MESH)
    pl.semaphore_wait(barrier, n)


def route_kernel(capacity, rows, depth, span, local_top, ids_ref, rw_ref, q_ref, pos_ref, msg_ref, top_ref, topw_ref):
    experts, chunk = LANES, 256
    tokens = ids_ref.shape[1]
    n_dest = msg_ref.shape[0]
    pitch = rows + TAIL
    before = (iota((chunk, chunk), 0) < iota((chunk, chunk), 1)).astype(bf16)
    expert_id = iota((experts, chunk), 0)
    slot_id = iota((span, chunk), 0)
    half_id = iota((n_dest, chunk), 0) * 2
    seen = jnp.zeros((experts, 1), f32)
    for c in range(tokens // chunk):
        at = slice(c * chunk, (c + 1) * chunk)
        hits = [expert_id == ids_ref[j:j + 1, at] for j in range(2)]
        member = jnp.where(hits[0] | hits[1], 1.0, 0.0)
        earlier = nn(member.astype(bf16), before) + seen
        seen = seen + across(member)
        for j in range(2):
            pos_ref[j:j + 1, at] = down(only(hits[j], earlier)).astype(i32)
    expert_col = iota((experts, 1), 0).astype(f32)
    kept = jnp.minimum(seen, float(capacity))
    if local_top:
        most = jnp.max(seen, axis=0, keepdims=True)
        top = jnp.min(jnp.where(seen == most, expert_col, float(experts)), axis=0, keepdims=True)
        kept = jnp.where(expert_col == top, 0.0, kept)
    else:
        top = jnp.full((1, 1), -1.0, f32)
    top_i = top.astype(i32)
    gates = [jnp.zeros((3 * n_dest, span), f32) for _ in range(2)]
    top_gates = jnp.zeros((24, LANES), f32)
    for c in range(tokens // chunk):
        at = slice(c * chunk, (c + 1) * chunk)
        for j in range(2):
            ids = ids_ref[j:j + 1, at]
            place = pos_ref[j:j + 1, at]
            weight = rw_ref[j:j + 1, at]
            keep = place < capacity
            slot = jnp.where(ids % 2 == 0, place, rows - 1 - place)
            q = (ids // 2) * pitch + slot
            if local_top:
                is_top = ids == top_i
                q = jnp.where(is_top, n_dest * pitch + place, q)
                slot = jnp.where(is_top, FAR, slot)
                top_hot = hot((iota((LANES, chunk), 0) == place) & keep & is_top)
                top_parts = [jnp.broadcast_to(p, (8, chunk)) for p in split3(weight)]
                top_gates = top_gates + nt(jnp.concatenate(top_parts, axis=0), top_hot)
            q_ref[j:j + 1, at] = jnp.where(keep, q, FAR)
            slot_hot = hot(slot_id == jnp.where(keep, slot, FAR))
            for par in range(2):
                mine = only(half_id + par == ids, weight)
                gates[par] = gates[par] + nt(jnp.concatenate(split3(mine), axis=0), slot_hot)
    kept_wide = jnp.broadcast_to(kept, (experts, LANES)).astype(bf16)
    owner = (iota((n_dest, experts), 1) // 2 == iota((n_dest, experts), 0)).astype(bf16)
    over = jnp.max(jnp.where(nn(owner, kept_wide) > float(rows), 1.0, 0.0), axis=0, keepdims=True)
    over = jnp.maximum(over, jnp.max(jnp.where(kept > float(depth), 1.0, 0.0), axis=0, keepdims=True))
    for par in range(2):
        g = gates[par]
        msg_ref[:, par * span:(par + 1) * span] = g[:n_dest] + g[n_dest:2 * n_dest] + g[2 * n_dest:]
    note = jnp.where(iota((1, LANES), 1) == 1, top, over)
    msg_ref[:, 2 * span:] = jnp.broadcast_to(note, (n_dest, LANES))
    top_ref[...] = jnp.broadcast_to(top_i, (8, LANES))
    topw_ref[...] = top_gates[:8] + top_gates[8:16] + top_gates[16:]


def pack_kernel(group, rows, first, q_ref, x_ref, dy_ref, out_ref):
    d = x_ref.shape[1]
    count, tokens = group * rows, q_ref.shape[1]
    row = iota((count, tokens), 0)
    slot = row + (row // rows + pl.program_id(0) * group) * TAIL + pl.program_id(0) * count + first
    pick = hot((q_ref[0:1, :] == slot) | (q_ref[1:2, :] == slot))
    out_ref[:, :d] = nn(pick, x_ref[...]).astype(bf16)
    out_ref[:, d:] = nn(pick, dy_ref[...]).astype(bf16)


def swiglu_rows(x, dy, weight, w1, w3, w2):
    h1 = nn(x, w1)
    h3 = nn(x, w3)
    s = jax.nn.sigmoid(h1)
    hidden = (h1 * s * h3).astype(bf16)
    dr = across(dy * nn(hidden, w2))
    g = (weight * dy).astype(bf16)
    da = nt(g, w2)
    dh1 = (da * h3 * s * (1.0 + h1 * (1.0 - s))).astype(bf16)
    dh3 = (da * h1 * s).astype(bf16)
    return hidden, g, dh1, dh3, nt(dh1, w1) + nt(dh3, w3), dr


def expert_body(depth, span, step, xdy_ref, rec_ref, w1_ref, w3_ref, w2_ref, dx_ref, dwg_ref, dwu_ref, dwd_ref):
    group, rows, width = xdy_ref.shape
    n_src = rec_ref.shape[0]
    d = width // 2
    m = group * depth

    local = iota((m, n_src), 0) // depth
    src_hot = hot(local + step * group == iota((m, n_src), 1))
    row_hot = hot(iota((m, LANES), 0) // depth == iota((m, LANES), 1))
    within = iota((m, span), 0) % depth
    outs, dr_slots = [], jnp.zeros((LANES, span), f32)
    for k in range(2):
        first = 0 if k == 0 else rows - depth
        slot_hot = iota((m, span), 1) == within + first
        gate_parts = jnp.concatenate(split3(rec_ref[:, k * span:(k + 1) * span]), axis=1)
        weight = across(only(slot_hot, add3(nn(src_hot, gate_parts), span)))
        x = xdy_ref[:, first:first + depth, :d].reshape(m, d)
        dy = xdy_ref[:, first:first + depth, d:].reshape(m, d).astype(f32)
        hidden, g, dh1, dh3, dx, dr = swiglu_rows(x, dy, weight, w1_ref[k], w3_ref[k], w2_ref[k])
        outs.append(dx.reshape(group, depth, d))
        dwg_ref[k] += tn(x, dh1)
        dwu_ref[k] += tn(x, dh3)
        dwd_ref[k] += tn(hidden, g)
        parts = jnp.concatenate(split3(only(slot_hot & (weight > 0.0), dr)), axis=1)
        dr_slots = dr_slots + add3(tn(row_hot, parts), span)
    low = rows - depth
    dx_ref[:, :low] = outs[0][:, :low].astype(bf16)
    if depth > low:
        dx_ref[:, low:depth] = (outs[0][:, low:] + outs[1][:, :depth - low]).astype(bf16)
    dx_ref[:, depth:rows] = outs[1][:, depth - low:].astype(bf16)
    parts = split3(dr_slots)
    for i in range(group):
        dx_ref[i, rows:, :] = jnp.zeros((TAIL, d), bf16)
        for n in range(3):
            dx_ref[i, rows + n:rows + n + 1, :span] = parts[n][i:i + 1, :]


def gather_weights(part, own, other, full):
    for mine, theirs, whole_ref, by_rows in zip(own, other, full, (True, True, False)):
        size = mine.shape[1] if by_rows else mine.shape[2]
        for ref, at in ((mine, part * size), (theirs, (1 - part) * size)):
            at = pl.ds(pl.multiple_of(at, LANES), size)
            for k in range(2):
                if by_rows:
                    whole_ref[k, at, :] = ref[k]
                else:
                    whole_ref[k, :, at] = ref[k]


def expert_kernel(depth, span, part_ref, xdy_ref, rec_ref, *refs):
    own, other, (dx_ref, dwg_ref, dwu_ref, dwd_ref), full = refs[:3], refs[3:6], refs[6:10], refs[10:]
    step = pl.program_id(0)

    @pl.when(step == 0)
    def _():
        for ref in (dwg_ref, dwu_ref, dwd_ref):
            ref[...] = jnp.zeros_like(ref)
        gather_weights(part_ref[0], own, other, full)

    expert_body(depth, span, step, xdy_ref, rec_ref, *full, dx_ref, dwg_ref, dwu_ref, dwd_ref)


def expert_send_kernel(depth, span, group, xdy_ref, rec_ref, *refs):
    own, other, dws, back_ref, peers, full = refs[:3], refs[3:6], refs[6:9], refs[9], refs[10:13], refs[13:16]
    dx_buf, ssem, rsem, psem, own_sem = refs[16:]
    me, part = lax.axis_index("ep"), lax.axis_index("fsdp")
    n = xdy_ref.shape[0]
    meet_all(me, part)
    for ref in dws:
        ref[...] = jnp.zeros_like(ref)
    gather_weights(part, own, other, full)

    def send(r):
        return pltpu.make_async_remote_copy(
            src_ref=dx_buf.at[r], dst_ref=back_ref.at[me], send_sem=ssem.at[r], recv_sem=rsem.at[r],
            device_id={"ep": peer_at(me, r, -1)}, device_id_type=MESH)

    keep = pltpu.make_async_copy(dx_buf.at[0], back_ref.at[me], own_sem)

    @pl.loop(0, n // group)
    def _(step):
        at = pl.ds(step * group, group)
        expert_body(depth, span, step, xdy_ref.at[at], rec_ref, *full, dx_buf.at[at], *dws)
        for j in range(group):
            if j == 0:
                @pl.when(step == 0)
                def _():
                    keep.start()

                @pl.when(step > 0)
                def _():
                    send(step * group).start()
            else:
                send(step * group + j).start()

    swaps = []
    for i, (dw, peer) in enumerate(zip(dws, peers)):
        size = peer.shape[1] if i < 2 else peer.shape[2]
        at = pl.ds(pl.multiple_of((1 - part) * size, LANES), size)
        swaps.append(pltpu.make_async_remote_copy(
            src_ref=dw.at[:, at, :] if i < 2 else dw.at[:, :, at], dst_ref=peer,
            send_sem=psem.at[0, i], recv_sem=psem.at[1, i], device_id={"fsdp": 1 - part}, device_id_type=MESH))
    for copy in swaps:
        copy.start()
    for copy in swaps:
        copy.wait()
    keep.wait()

    @pl.loop(1, n)
    def _(r):
        send(r).wait()


def dispatch_kernel(group, q_ref, x_ref, dy_ref, msg_ref, wm_ref, gate_ref,
                    xdy_ref, rec_ref, dx_ref, dr_ref, grad_ref,
                    packed, rows_ref, wbuf, wr0, wr1, wr2, wfull, gfull, gbuf, gpeer, gr0, gr1, gr2,
                    bsem, msem, ssem, rsem, own_sem):
    me, part = lax.axis_index("ep"), lax.axis_index("fsdp")
    coord = coords(me)
    n_mat, total = wbuf.shape[0], wbuf.shape[1]
    levels = len(STRIDES)
    n_dest, rows, _ = xdy_ref.shape
    d, tokens = x_ref.shape[1], x_ref.shape[0]
    pitch = rows + TAIL
    meet_all(me, part)

    def pack(slot):
        pick = hot((q_ref[0:1, :] == slot) | (q_ref[1:2, :] == slot))
        return nn(pick, x_ref[...]).astype(bf16), nn(pick, dy_ref[...]).astype(bf16)

    def block_copies(r):
        to = peer_at(me, r, 1)
        return [pltpu.make_async_remote_copy(
                    src_ref=packed.at[r], dst_ref=xdy_ref.at[r], send_sem=bsem.at[0, r], recv_sem=bsem.at[1, r],
                    device_id={"ep": to}, device_id_type=MESH),
                pltpu.make_async_remote_copy(
                    src_ref=msg_ref.at[to], dst_ref=rec_ref.at[r], send_sem=msem.at[0, r], recv_sem=msem.at[1, r],
                    device_id={"ep": to}, device_id_type=MESH)]

    keep = [pltpu.make_async_copy(packed.at[0], xdy_ref.at[0], own_sem.at[0]),
            pltpu.make_async_copy(msg_ref.at[me], rec_ref.at[0], own_sem.at[1])]

    def send_blocks(step):
        line = iota((group * rows, 1), 0)
        slot = line
        for j in range(group):
            inside = (line >= j * rows) & (line < (j + 1) * rows)
            slot = jnp.where(inside, line - j * rows + peer_at(me, step * group + j, 1) * pitch, slot)
        x_rows, dy_rows = pack(slot)
        for j in range(group):
            at = slice(j * rows, (j + 1) * rows)
            packed[step * group + j, :, :d] = x_rows[at]
            packed[step * group + j, :, d:] = dy_rows[at]
        for j in range(group):
            if j == 0:
                @pl.when(step == 0)
                def _():
                    for copy in keep:
                        copy.start()

                @pl.when(step > 0)
                def _():
                    for copy in block_copies(step * group):
                        copy.start()
            else:
                for copy in block_copies(step * group + j):
                    copy.start()

    sizes = [total // SIDE ** (level + 1) for level in range(levels)]

    def base_of(c, level):
        base = 0
        for i in range(level):
            base = base + coord[(c + i) % 3] * sizes[i]
        return base

    def at(base, size):
        return pl.ds(pl.multiple_of(base, 16), size)

    def peer(axis, delta):
        return me + ((coord[axis] + delta) % SIDE - coord[axis]) * STRIDES[axis]

    w_put = lambda c, s: wfull.at[part, c, s]
    g_put = lambda c, s: grad_ref.at[c, s]
    plans = ((wbuf, (wr0, wr1, wr2), w_put), (gbuf, (gr0, gr1, gr2), g_put))

    def scatter_copies(which, level):
        buf, recvs, _ = plans[which]
        out = []
        for c in range(n_mat):
            axis = (c + level) % 3
            for delta in (1, 2, 3):
                to = (coord[axis] + delta) % SIDE
                out.append(pltpu.make_async_remote_copy(
                    src_ref=buf.at[c, at(base_of(c, level) + to * sizes[level], sizes[level])],
                    dst_ref=recvs[level].at[c, 3 - delta],
                    send_sem=ssem.at[which, 0, level, c, delta - 1], recv_sem=rsem.at[which, 0, level, c, 3 - delta],
                    device_id={"ep": peer(axis, delta)}, device_id_type=MESH))
        return out

    def scatter_add(which, level):
        buf, recvs, put = plans[which]
        for c in range(n_mat):
            mine = at(base_of(c, level + 1), sizes[level])
            got = [recvs[level][c, i].astype(f32) for i in range(3)]
            value = (buf[c, mine].astype(f32) + got[0] + got[1] + got[2]).astype(buf.dtype)
            if level == levels - 1:
                put(c, mine)[...] = value
            else:
                buf[c, mine] = value

    def gather_copies(which, level):
        put = plans[which][2]
        out = []
        for c in range(n_mat):
            axis = (c + level) % 3
            mine = at(base_of(c, level + 1), sizes[level])
            for delta in (1, 2, 3):
                out.append(pltpu.make_async_remote_copy(
                    src_ref=put(c, mine), dst_ref=put(c, mine),
                    send_sem=ssem.at[which, 1, level, c, delta - 1], recv_sem=rsem.at[which, 1, level, c, 3 - delta],
                    device_id={"ep": peer(axis, delta)}, device_id_type=MESH))
        return out

    def swap_copies(which):
        src, dst = ((wfull.at[part], wfull.at[part]), (gfull.at[1 - part], gpeer))[which]
        return [pltpu.make_async_remote_copy(
            src_ref=src, dst_ref=dst, send_sem=ssem.at[which, 2, 0, 0, 0], recv_sem=rsem.at[which, 2, 0, 0, 0],
            device_id={"fsdp": 1 - part}, device_id_type=MESH)]

    def serve_top():
        half, wide = d // 2, d // LANES
        mats = []
        for i in range(2):
            mats.append(jnp.concatenate([jnp.concatenate(
                [wfull[f, i, b * half:(b + 1) * half, :] for b in range(wide)], axis=1) for f in range(2)], axis=0))
        w2 = jnp.concatenate([wfull[f, 2, b * d:(b + 1) * d, :] for f in range(2) for b in range(wide // 2)], axis=1)
        n = rows_ref.shape[0]
        x = rows_ref[:, :d]
        dy = rows_ref[:, d:].astype(f32)
        eye = iota((n, n), 0) == iota((n, n), 1)
        weight = across(only(eye, gate_ref[0:1, :]))
        hidden, g, dh1, dh3, dx, dr = swiglu_rows(x, dy, weight, mats[0], mats[1], w2)
        dx_ref[...] = dx.astype(bf16)
        dr_ref[...] = jnp.broadcast_to(dr, dr_ref.shape)
        for i, dh in enumerate((dh1, dh3)):
            dw = tn(x, dh)
            for f in range(2):
                for b in range(wide):
                    gfull[f, i, b * half:(b + 1) * half, :] = dw[f * half:(f + 1) * half, b * LANES:(b + 1) * LANES]
        dw = tn(hidden, g)
        for f in range(2):
            for b in range(wide // 2):
                lane = f * half + b * LANES
                gfull[f, 2, b * d:(b + 1) * d, :] = dw[:, lane:lane + LANES]

    def fold_peer():
        gbuf[...] = gfull[part] + gpeer[...]

    phases = []
    for which in range(2):
        if which == 1:
            phases.append((lambda: swap_copies(1), fold_peer))
        for level in range(levels):
            phases.append((functools.partial(scatter_copies, which, level), functools.partial(scatter_add, which, level)))
        for level in reversed(range(levels)):
            phases.append((functools.partial(gather_copies, which, level), None))
        if which == 0:
            phases.append((lambda: swap_copies(0), serve_top))

    wbuf[...] = wm_ref[...]
    x_rows, dy_rows = pack(iota((rows_ref.shape[0], 1), 0) + n_dest * pitch)
    rows_ref[:, :d] = x_rows
    rows_ref[:, d:] = dy_rows
    steps = n_dest // group

    @pl.loop(0, steps)
    def _(step):
        for i, (copies, _) in enumerate(phases):
            @pl.when(step == i)
            def _(copies=copies):
                for copy in copies():
                    copy.start()

        send_blocks(step)

        for i, (copies, then) in enumerate(phases):
            @pl.when(step == i)
            def _(copies=copies, then=then):
                for copy in copies():
                    copy.wait()
                if then is not None:
                    then()

    for copy in keep:
        copy.wait()

    @pl.loop(1, n_dest)
    def _(r):
        for copy in block_copies(r):
            copy.wait()


def dr_kernel(rows, span, ids_ref, q_ref, pos_ref, back_ref, top_dr_ref, out_ref):
    n_src = back_ref.shape[0]
    tokens = ids_ref.shape[1]
    pitch = rows + TAIL
    chunk = 512
    tables = [back_ref[:, n, :span].T for n in range(3)]
    for c in range(tokens // chunk):
        at = slice(c * chunk, (c + 1) * chunk)
        for j in range(2):
            block = ids_ref[j:j + 1, at] // 2
            q = q_ref[j:j + 1, at]
            owner = hot(iota((n_src, chunk), 0) == block)
            column = nn(tables[0], owner) + nn(tables[1], owner) + nn(tables[2], owner)
            far = q >= n_src * pitch
            want = jnp.where(far, FAR, q - block * pitch)
            picked = down(only(iota((span, chunk), 0) == want, column))
            if top_dr_ref is not None:
                want = jnp.where(far, q - n_src * pitch, FAR)
                picked = picked + down(
                    only(iota((LANES, chunk), 0) == want, top_dr_ref[:, 0:1]))
            out_ref[j:j + 1, at] = picked


def combine_kernel(q_ref, back_ref, *rest):
    top_ref, out_ref = rest if len(rest) == 2 else (None, rest[0])
    rows, slots = q_ref.shape[0], back_ref.shape[0]
    q0, q1 = q_ref[:, 0:1], q_ref[:, 1:2]
    acc = jnp.zeros(out_ref.shape, f32)
    for at in range(0, slots, 512):
        depth = min(512, slots - at)
        column = iota((rows, depth), 1) + at
        pick = hot((q0 == column) | (q1 == column))
        acc = acc + nn(pick, back_ref[at:at + depth, :])
    if top_ref is not None:
        column = iota((rows, LANES), 1) + slots
        pick = hot((q0 == column) | (q1 == column))
        acc = acc + nn(pick, top_ref[...])
    out_ref[...] = acc.astype(bf16)


def vmem():
    return pl.BlockSpec(memory_space=pltpu.VMEM)


def whole(shape):
    return pl.BlockSpec(shape, lambda i: (0,) * len(shape))


PARAMS = pltpu.CompilerParams(vmem_limit_bytes=60 * 1024 * 1024)


def exchange(v):
    return lax.all_to_all(v, "ep", 0, 0, tiled=True)


ANYWHERE = pl.BlockSpec(memory_space=pl.ANY)


def dispatch(q_t, x_tok, dy_tok, msg, w_mine, gate, n_dest, rows):
    d, n_mat, total = x_tok.shape[1], 3, w_mine.shape[1]
    scratch = [pltpu.VMEM((n_dest, rows, 2 * d), bf16), pltpu.VMEM((LANES, 2 * d), bf16)]
    for dtype in (bf16, f32):
        recvs = [pltpu.VMEM((n_mat, 3, total // 4 ** (i + 1), LANES), dtype) for i in range(3)]
        if dtype == bf16:
            scratch += [pltpu.VMEM((n_mat, total, LANES), dtype), *recvs, pltpu.VMEM((2, n_mat, total, LANES), dtype)]
        else:
            scratch += [pltpu.VMEM((2, n_mat, total, LANES), dtype), pltpu.VMEM((n_mat, total, LANES), dtype),
                        pltpu.VMEM((n_mat, total, LANES), dtype), *recvs]
    dma = pltpu.SemaphoreType.DMA
    scratch += [dma((2, n_dest)), dma((2, n_dest)), dma((2, 3, 3, n_mat, 3)), dma((2, 3, 3, n_mat, 3)), dma((2,))]
    return pl.pallas_call(
        functools.partial(dispatch_kernel, 4),
        out_shape=(jax.ShapeDtypeStruct((n_dest, rows, 2 * d), bf16),
                   jax.ShapeDtypeStruct(msg.shape, f32),
                   jax.ShapeDtypeStruct((LANES, d), bf16),
                   jax.ShapeDtypeStruct((LANES, LANES), f32),
                   jax.ShapeDtypeStruct((n_mat, total, LANES), f32)),
        in_specs=[vmem()] * 6, out_specs=(ANYWHERE, vmem(), vmem(), vmem(), vmem()), scratch_shapes=scratch,
        compiler_params=pltpu.CompilerParams(
            vmem_limit_bytes=60 * 1024 * 1024, collective_id=0, has_side_effects=True),
        cost_estimate=pl.CostEstimate(flops=100_000_000_000, bytes_accessed=30_000_000, transcendentals=0),
        name="dispatch",
    )(q_t, x_tok, dy_tok, msg, w_mine, gate)


class Plan:
    def __init__(self, rows, depth, pack_group, group, capacity, n_ep, local_top):
        self.rows, self.depth, self.pack_group, self.group = rows, depth, pack_group, group
        self.capacity, self.n_ep, self.local_top = capacity, n_ep, local_top
        self.span = -(-rows // LANES) * LANES

    def pack(self, q_t, x_tok, dy_tok, group, rows, steps, first):
        tok_dev, d = x_tok.shape
        return pl.pallas_call(
            functools.partial(pack_kernel, group, rows, first),
            out_shape=jax.ShapeDtypeStruct((steps * group * rows, 2 * d), bf16),
            grid=(steps,),
            in_specs=[whole((2, tok_dev)), whole((tok_dev, d)), whole((tok_dev, d))],
            out_specs=pl.BlockSpec((group * rows, 2 * d), lambda i: (i, 0)),
            compiler_params=PARAMS, name="pack",
        )(q_t, x_tok, dy_tok)

    def route(self, ids_t, rw_t):
        n_ep, rows, span, tok_dev = self.n_ep, self.rows, self.span, ids_t.shape[1]
        q_t, _, msg, top, gate = pl.pallas_call(
            functools.partial(route_kernel, self.capacity, rows, self.depth, span, self.local_top),
            out_shape=(jax.ShapeDtypeStruct((2, tok_dev), i32), jax.ShapeDtypeStruct((2, tok_dev), i32),
                       jax.ShapeDtypeStruct((n_ep, 2 * span + LANES), f32),
                       jax.ShapeDtypeStruct((8, LANES), i32), jax.ShapeDtypeStruct((8, LANES), f32)),
            in_specs=[vmem(), vmem()], out_specs=(vmem(),) * 5, compiler_params=PARAMS, name="route",
        )(ids_t, rw_t)
        return q_t, msg, top, gate

    def forward(self, me, part, x_tok, dy_tok, ids_t, rw_t, weights, own):
        d = x_tok.shape[1]
        n_ep, rows = self.n_ep, self.rows
        q_t, msg, _, _ = self.route(ids_t, rw_t)
        rec = exchange(msg)
        packed = self.pack(q_t, x_tok, dy_tok, self.pack_group, rows, n_ep // self.pack_group, 0)
        xdy = exchange(packed.reshape(n_ep, rows, 2 * d))
        dx, *dws = self.experts(part, xdy, rec, weights, own)
        return q_t, exchange(dx), dws

    def forward_top(self, me, part, x_tok, dy_tok, ids_t, rw_t, weights, own):
        n_ep, rows, span = self.n_ep, self.rows, self.span
        q_t, msg, top, gate = self.route(ids_t, rw_t)
        top_id = top[0, 0]
        mine = top_id // 2 == me
        flat = []
        for w in own:
            one = lax.dynamic_index_in_dim(w, top_id % 2, 0, keepdims=False)
            one = jnp.where(mine, one, jnp.zeros_like(one))
            flat.append(one.reshape(one.shape[0], -1, LANES).transpose(1, 0, 2).reshape(-1, LANES))
        xdy, rec, top_dx, top_dr, top_grad = dispatch(
            q_t, x_tok, dy_tok, msg.reshape(n_ep, 1, -1), jnp.stack(flat), gate, n_ep, rows)
        rec = rec.reshape(n_ep, -1)
        dws, back, peers = self.experts_send(xdy, rec, weights, own)
        return rec[:, 2 * span:], q_t, back, (top_id, top_dx, top_dr, top_grad), dws, peers

    def experts(self, part, xdy, rec, weights, own):
        n_ep, rows, width = xdy.shape
        d, group, span = width // 2, self.group, self.span
        ff = own[0].shape[2]
        return pl.pallas_call(
            functools.partial(expert_kernel, self.depth, span),
            out_shape=(jax.ShapeDtypeStruct((n_ep, rows + TAIL, d), bf16),
                       jax.ShapeDtypeStruct((2, d, ff), f32),
                       jax.ShapeDtypeStruct((2, d, ff), f32),
                       jax.ShapeDtypeStruct((2, ff, d), f32)),
            grid=(n_ep // group,),
            in_specs=[pl.BlockSpec(memory_space=pltpu.SMEM), pl.BlockSpec((group, rows, width), lambda i: (i, 0, 0)),
                      whole(rec.shape)] + [whole(w.shape) for w in (*own, *weights)],
            out_specs=(pl.BlockSpec((group, rows + TAIL, d), lambda i: (i, 0, 0)),
                       whole((2, d, ff)), whole((2, d, ff)), whole((2, ff, d))),
            scratch_shapes=[pltpu.VMEM((2, d, ff), bf16), pltpu.VMEM((2, d, ff), bf16), pltpu.VMEM((2, ff, d), bf16)],
            compiler_params=PARAMS, name="experts",
        )(part.reshape(1), xdy, rec, *own, *weights)

    def experts_send(self, xdy, rec, weights, own):
        n_ep, rows, width = xdy.shape
        d, ff = width // 2, own[0].shape[2]
        pitch = rows + TAIL
        dma = pltpu.SemaphoreType.DMA
        out = pl.pallas_call(
            functools.partial(expert_send_kernel, self.depth, self.span, self.group),
            out_shape=(jax.ShapeDtypeStruct((2, d, ff), f32), jax.ShapeDtypeStruct((2, d, ff), f32),
                       jax.ShapeDtypeStruct((2, ff, d), f32), jax.ShapeDtypeStruct((n_ep, pitch, d), bf16),
                       *(jax.ShapeDtypeStruct(w.shape, f32) for w in own)),
            in_specs=[vmem()] * 8, out_specs=(vmem(),) * 3 + (ANYWHERE,) * 4,
            scratch_shapes=[pltpu.VMEM((2, d, ff), bf16), pltpu.VMEM((2, d, ff), bf16), pltpu.VMEM((2, ff, d), bf16),
                            pltpu.VMEM((n_ep, pitch, d), bf16), dma((n_ep,)), dma((n_ep,)), dma((2, 3)), dma],
            compiler_params=pltpu.CompilerParams(
                vmem_limit_bytes=60 * 1024 * 1024, collective_id=1, has_side_effects=True),
            cost_estimate=pl.CostEstimate(flops=60_000_000_000, bytes_accessed=30_000_000, transcendentals=0),
            name="experts_send",
        )(xdy, rec, *own, *weights)
        return out[:3], out[3], out[4:]

    def finish(self, ids_t, q_t, back, top_out):
        tok_dev, (n_ep, pitch, d), tile = q_t.shape[1], back.shape, 256
        tail = back[:, self.rows:, :]
        dr_args = [ids_t, q_t, q_t, tail] + ([top_out[2]] if top_out else [])
        kernel = functools.partial(dr_kernel, self.rows, self.span)
        if not top_out:
            inner = kernel
            kernel = lambda a, b, c, e, out: inner(a, b, c, e, None, out)
        dr_t = pl.pallas_call(
            kernel, out_shape=jax.ShapeDtypeStruct((2, tok_dev), f32),
            in_specs=[vmem()] * len(dr_args), out_specs=vmem(), compiler_params=PARAMS, name="route_grad",
        )(*dr_args)
        slots = n_ep * pitch
        args = [q_t.T, back.reshape(slots, d)] + ([top_out[1]] if top_out else [])
        grad_x = pl.pallas_call(
            combine_kernel,
            out_shape=jax.ShapeDtypeStruct((tok_dev, d), bf16),
            grid=(tok_dev // tile,),
            in_specs=[pl.BlockSpec((tile, 2), lambda i: (i, 0))] + [whole(v.shape) for v in args[1:]],
            out_specs=pl.BlockSpec((tile, d), lambda i: (i, 0)),
            compiler_params=PARAMS, name="combine",
        )(*args)
        return grad_x, dr_t.T


def solution(mesh):
    n_ep = mesh.shape["ep"]
    tok_spec = P(("fsdp", "ep"), None)
    spec_in = P("ep", "fsdp", None)
    spec_out = P("ep", None, "fsdp")

    def per_device(x_tok, dy_tok, expert_ids, route_w, w_gate, w_up, w_down):
        tok_dev, top_k = expert_ids.shape
        capacity = capacity_of(tok_dev, top_k, w_gate.shape[0] * n_ep)
        me, part = lax.axis_index("ep").astype(i32), lax.axis_index("fsdp").astype(i32)
        swap = [(0, 1), (1, 0)]
        own = (w_gate, w_up, w_down)
        weights = [lax.ppermute(w, "fsdp", swap) for w in own]
        ids_t = expert_ids.T
        inputs = (me, part, x_tok, dy_tok, ids_t, route_w.T, weights, own)

        def shard_halves(dws):
            out = []
            for dw, axis in zip(dws, (1, 1, 2)):
                size = dw.shape[axis] // 2
                keep = lax.dynamic_slice_in_dim(dw, part * size, size, axis)
                give = lax.dynamic_slice_in_dim(dw, (1 - part) * size, size, axis)
                out.append(keep + lax.ppermute(give, "fsdp", swap))
            return out

        quick = Plan(72, 48, 4, 8, capacity, n_ep, True)
        safe = Plan(2 * capacity, capacity, 2, 4, capacity, n_ep, False)
        notes, q_t, back, top_out, dws, peers = quick.forward_top(*inputs)
        top_id = top_out[0]
        agree = jnp.all(notes[:, 1] == top_id.astype(f32)) & jnp.all(notes[:, 0] == 0.0)
        note = jnp.where(agree, top_id.astype(f32), -1.0).reshape(1, 1)
        other = lax.ppermute(note, "fsdp", swap)
        good = agree & (other == note)[0, 0]

        def fits():
            grads = []
            for i, (dw, peer) in enumerate(zip(dws, peers)):
                axis = 1 if i < 2 else 2
                size = peer.shape[axis]
                half = lax.dynamic_slice_in_dim(dw, part * size, size, axis) + peer
                rows = half.shape[1]
                extra = top_out[3][i].reshape(-1, rows, LANES).transpose(1, 0, 2).reshape(1, *half.shape[1:])
                pick = (jnp.arange(2) + 2 * me == top_id)[:, None, None]
                grads.append(half + only(pick, extra))
            return (*quick.finish(ids_t, q_t, back, top_out), *grads)

        def general():
            q_all, back_all, dw_all = safe.forward(*inputs)
            return (*safe.finish(ids_t, q_all, back_all, None), *shard_halves(dw_all))

        return lax.cond(good, fits, general)

    return jax.shard_map(
        per_device, mesh=mesh,
        in_specs=(tok_spec, tok_spec, tok_spec, tok_spec, spec_in, spec_in, spec_out),
        out_specs=(tok_spec, tok_spec, spec_in, spec_in, spec_out),
        check_vma=False)
```

```python
import functools

import jax
import jax.numpy as jnp
from jax import lax
from jax.experimental import pallas as pl
from jax.experimental.pallas import tpu as pltpu
from jax.sharding import PartitionSpec as P

CAP_FACTOR = 3
LANES = 128
FAR = 1 << 20
MESH = pl.DeviceIdType.MESH
f32, bf16, i32 = jnp.float32, jnp.bfloat16, jnp.int32


def capacity_of(tok_dev, top_k, experts):
    return max(8, ((CAP_FACTOR * tok_dev * top_k // experts + 7) // 8) * 8)


def iota(shape, dim):
    return lax.broadcasted_iota(i32, shape, dim)


def nn(a, b):
    return jnp.dot(a, b, preferred_element_type=f32)


def nt(a, b):
    return lax.dot_general(a, b, (((1,), (1,)), ((), ())), preferred_element_type=f32)


def tn(a, b):
    return lax.dot_general(a, b, (((0,), (0,)), ((), ())), preferred_element_type=f32)


def split3(v):
    hi = v.astype(bf16)
    rest = v - hi.astype(f32)
    mid = rest.astype(bf16)
    lo = (rest - mid.astype(f32)).astype(bf16)
    return hi, mid, lo


def hot(mask):
    return jnp.where(mask, 1.0, 0.0).astype(bf16)


def only(mask, v):
    return jnp.where(mask, v, jnp.zeros_like(v))


def down(v):
    return jnp.sum(v, axis=0, keepdims=True)


def across(v):
    return jnp.sum(v, axis=1, keepdims=True)


def add3(v, n):
    return v[:, :n] + v[:, n:2 * n] + v[:, 2 * n:]


SIDE = 4
STRIDES = (1, SIDE, SIDE * SIDE)


def coords(me):
    return [me % SIDE, (me // SIDE) % SIDE, me // (SIDE * SIDE)]


def peer_at(me, r, sign):
    o = (r * 23) % SIDE ** 3
    out = 0
    for here, off, stride in zip(coords(me), coords(o), STRIDES):
        out = out + ((here + sign * off + SIDE) % SIDE) * stride
    return out


def meet_all(me, part):
    barrier = pltpu.get_barrier_semaphore()
    n = SIDE ** 3

    @pl.loop(1, n)
    def _(r):
        pl.semaphore_signal(barrier, inc=1, device_id={"ep": peer_at(me, r, 1)}, device_id_type=MESH)

    pl.semaphore_signal(barrier, inc=1, device_id={"fsdp": 1 - part}, device_id_type=MESH)
    pl.semaphore_wait(barrier, n)


def remote(src, dst, sems, at, to, back=None):
    return pltpu.make_async_remote_copy(
        src_ref=src, dst_ref=dst, send_sem=sems.at[(0, *at)], recv_sem=sems.at[(1, *(back or at))],
        device_id=to, device_id_type=MESH)


def start_blocks(step, group, copies, keep):
    for j in range(group):
        if j == 0:
            @pl.when(step == 0)
            def _():
                for copy in keep:
                    copy.start()

            @pl.when(step > 0)
            def _():
                for copy in copies(step * group):
                    copy.start()
        else:
            for copy in copies(step * group + j):
                copy.start()


def wait_blocks(n, copies, keep):
    for copy in keep:
        copy.wait()

    @pl.loop(1, n)
    def _(r):
        for copy in copies(r):
            copy.wait()


def in_step(steps, phases, work):
    @pl.loop(0, steps)
    def _(step):
        for i, (copies, _) in enumerate(phases):
            @pl.when(step == i)
            def _(copies=copies):
                for copy in copies():
                    copy.start()

        work(step)

        for i, (copies, then) in enumerate(phases):
            @pl.when(step == i)
            def _(copies=copies, then=then):
                for copy in copies():
                    copy.wait()
                if then is not None:
                    then()


def all_reduce(me, buf, recvs, put, sems_out, sems_in):
    coord = coords(me)
    n_mat, total = buf.shape[0], buf.shape[1]
    levels = len(STRIDES)
    sizes = [total // SIDE ** (level + 1) for level in range(levels)]

    def at(base, size):
        return pl.ds(pl.multiple_of(base, 16), size)

    def base_of(c, level):
        base = 0
        for i in range(level):
            base = base + coord[(c + i) % levels] * sizes[i]
        return base

    def lines(level):
        for c in range(n_mat):
            axis = (c + level) % levels
            for delta in range(1, SIDE):
                to = (coord[axis] + delta) % SIDE
                yield c, delta, to, {"ep": me + (to - coord[axis]) * STRIDES[axis]}

    def scatter(level):
        return [remote(buf.at[c, at(base_of(c, level) + to * sizes[level], sizes[level])], recvs[level].at[c, 3 - delta],
                       sems_out, (level, c, delta - 1), peer, (level, c, 3 - delta))
                for c, delta, to, peer in lines(level)]

    def gather(level):
        out = []
        for c, delta, _, peer in lines(level):
            mine = put(c, at(base_of(c, level + 1), sizes[level]))
            out.append(remote(mine, mine, sems_in, (level, c, delta - 1), peer, (level, c, 3 - delta)))
        return out

    def add(level):
        for c in range(n_mat):
            mine = at(base_of(c, level + 1), sizes[level])
            value = buf[c, mine].astype(f32)
            for i in range(SIDE - 1):
                value = value + recvs[level][c, i].astype(f32)
            if level == levels - 1:
                put(c, mine)[...] = value.astype(buf.dtype)
            else:
                buf[c, mine] = value.astype(buf.dtype)

    return ([(functools.partial(scatter, level), functools.partial(add, level)) for level in range(levels)]
            + [(functools.partial(gather, level), None) for level in reversed(range(levels))])


def route_kernel(capacity, rows, depth, span, local_top, ids_ref, rw_ref, q_ref, pos_ref, msg_ref, top_ref, topw_ref):
    experts, chunk = LANES, 256
    tokens = ids_ref.shape[1]
    n_dest = msg_ref.shape[0]
    before = (iota((chunk, chunk), 0) < iota((chunk, chunk), 1)).astype(bf16)
    expert_id = iota((experts, chunk), 0)
    slot_id = iota((span, chunk), 0)
    half_id = iota((n_dest, chunk), 0) * 2
    seen = jnp.zeros((experts, 1), f32)
    for c in range(tokens // chunk):
        at = slice(c * chunk, (c + 1) * chunk)
        hits = [expert_id == ids_ref[j:j + 1, at] for j in range(2)]
        member = jnp.where(hits[0] | hits[1], 1.0, 0.0)
        earlier = nn(member.astype(bf16), before) + seen
        seen = seen + across(member)
        for j in range(2):
            pos_ref[j:j + 1, at] = down(only(hits[j], earlier)).astype(i32)
    expert_col = iota((experts, 1), 0).astype(f32)
    kept = jnp.minimum(seen, float(capacity))
    if local_top:
        most = jnp.max(seen, axis=0, keepdims=True)
        top = jnp.min(jnp.where(seen == most, expert_col, float(experts)), axis=0, keepdims=True)
        kept = jnp.where(expert_col == top, 0.0, kept)
    else:
        top = jnp.full((1, 1), -1.0, f32)
    top_i = top.astype(i32)
    gates = [jnp.zeros((3 * n_dest, span), f32) for _ in range(2)]
    top_gates = jnp.zeros((24, LANES), f32)
    for c in range(tokens // chunk):
        at = slice(c * chunk, (c + 1) * chunk)
        for j in range(2):
            ids = ids_ref[j:j + 1, at]
            place = pos_ref[j:j + 1, at]
            weight = rw_ref[j:j + 1, at]
            keep = place < capacity
            slot = jnp.where(ids % 2 == 0, place, rows - 1 - place)
            q = (ids // 2) * rows + slot
            if local_top:
                is_top = ids == top_i
                q = jnp.where(is_top, n_dest * rows + place, q)
                slot = jnp.where(is_top, FAR, slot)
                top_hot = hot((iota((LANES, chunk), 0) == place) & keep & is_top)
                top_parts = [jnp.broadcast_to(p, (8, chunk)) for p in split3(weight)]
                top_gates = top_gates + nt(jnp.concatenate(top_parts, axis=0), top_hot)
            q_ref[j:j + 1, at] = jnp.where(keep, q, FAR)
            slot_hot = hot(slot_id == jnp.where(keep, slot, FAR))
            for par in range(2):
                mine = only(half_id + par == ids, weight)
                gates[par] = gates[par] + nt(jnp.concatenate(split3(mine), axis=0), slot_hot)
    kept_wide = jnp.broadcast_to(kept, (experts, LANES)).astype(bf16)
    owner = (iota((n_dest, experts), 1) // 2 == iota((n_dest, experts), 0)).astype(bf16)
    over = jnp.max(jnp.where(nn(owner, kept_wide) > float(rows), 1.0, 0.0), axis=0, keepdims=True)
    over = jnp.maximum(over, jnp.max(jnp.where(kept > float(depth), 1.0, 0.0), axis=0, keepdims=True))
    for par in range(2):
        g = gates[par]
        msg_ref[:, par * span:(par + 1) * span] = g[:n_dest] + g[n_dest:2 * n_dest] + g[2 * n_dest:]
    note = jnp.where(iota((1, LANES), 1) == 1, top, over)
    msg_ref[:, 2 * span:] = jnp.broadcast_to(note, (n_dest, LANES))
    top_ref[...] = jnp.broadcast_to(top_i, (8, LANES))
    topw_ref[...] = top_gates[:8] + top_gates[8:16] + top_gates[16:]


def pack_kernel(q_ref, x_ref, dy_ref, out_ref):
    d, count = x_ref.shape[1], out_ref.shape[0]
    slot = iota((count, 1), 0) + pl.program_id(0) * count
    pick = hot((q_ref[0:1, :] == slot) | (q_ref[1:2, :] == slot))
    out_ref[:, :d] = nn(pick, x_ref[...]).astype(bf16)
    out_ref[:, d:] = nn(pick, dy_ref[...]).astype(bf16)


def swiglu_rows(x, dy, weight, w1, w3, w2):
    h1 = nn(x, w1)
    h3 = nn(x, w3)
    s = jax.nn.sigmoid(h1)
    hidden = (h1 * s * h3).astype(bf16)
    dr = across(dy * nn(hidden, w2))
    g = (weight * dy).astype(bf16)
    da = nt(g, w2)
    dh1 = (da * h3 * s * (1.0 + h1 * (1.0 - s))).astype(bf16)
    dh3 = (da * h1 * s).astype(bf16)
    return hidden, g, dh1, dh3, nt(dh1, w1) + nt(dh3, w3), dr


def expert_body(depth, span, step, xdy_ref, rec_ref, w1_ref, w3_ref, w2_ref, dx_ref, dr_ref, dwg_ref, dwu_ref, dwd_ref):
    group, rows, width = xdy_ref.shape
    n_src = rec_ref.shape[0]
    d = width // 2
    m = group * depth

    local = iota((m, n_src), 0) // depth
    src_hot = hot(local + step * group == iota((m, n_src), 1))
    row_hot = hot(iota((m, LANES), 0) // depth == iota((m, LANES), 1))
    within = iota((m, span), 0) % depth
    outs, dr_slots = [], jnp.zeros((LANES, span), f32)
    for k in range(2):
        first = 0 if k == 0 else rows - depth
        slot_hot = iota((m, span), 1) == within + first
        gate_parts = jnp.concatenate(split3(rec_ref[:, k * span:(k + 1) * span]), axis=1)
        weight = across(only(slot_hot, add3(nn(src_hot, gate_parts), span)))
        x = xdy_ref[:, first:first + depth, :d].reshape(m, d)
        dy = xdy_ref[:, first:first + depth, d:].reshape(m, d).astype(f32)
        hidden, g, dh1, dh3, dx, dr = swiglu_rows(x, dy, weight, w1_ref[k], w3_ref[k], w2_ref[k])
        outs.append(dx.reshape(group, depth, d))
        dwg_ref[k] += tn(x, dh1)
        dwu_ref[k] += tn(x, dh3)
        dwd_ref[k] += tn(hidden, g)
        parts = jnp.concatenate(split3(only(slot_hot & (weight > 0.0), dr)), axis=1)
        dr_slots = dr_slots + add3(tn(row_hot, parts), span)
    low = rows - depth
    dx_ref[:, :low] = outs[0][:, :low].astype(bf16)
    if depth > low:
        dx_ref[:, low:depth] = (outs[0][:, low:] + outs[1][:, :depth - low]).astype(bf16)
    dx_ref[:, depth:] = outs[1][:, depth - low:].astype(bf16)
    for i in range(group):
        dr_ref[i] = dr_slots[i:i + 1]


def gather_weights(part, own, other, full):
    for mine, theirs, whole_ref, by_rows in zip(own, other, full, (True, True, False)):
        size = mine.shape[1] if by_rows else mine.shape[2]
        for ref, at in ((mine, part * size), (theirs, (1 - part) * size)):
            at = pl.ds(pl.multiple_of(at, LANES), size)
            for k in range(2):
                if by_rows:
                    whole_ref[k, at, :] = ref[k]
                else:
                    whole_ref[k, :, at] = ref[k]


def expert_kernel(depth, span, part_ref, xdy_ref, rec_ref, *refs):
    own, other, (dx_ref, dr_ref), dws, full = refs[:3], refs[3:6], refs[6:8], refs[8:11], refs[11:]
    step = pl.program_id(0)

    @pl.when(step == 0)
    def _():
        for ref in dws:
            ref[...] = jnp.zeros_like(ref)
        gather_weights(part_ref[0], own, other, full)

    expert_body(depth, span, step, xdy_ref, rec_ref, *full, dx_ref, dr_ref, *dws)


def expert_send_kernel(depth, span, group, xdy_ref, rec_ref, top_ref, gfull, *refs):
    own, other, back_ref, dr_back, outs = refs[:3], refs[3:6], refs[6], refs[7], refs[8:11]
    full, dws, peers = refs[11:14], refs[14:17], refs[17:20]
    dx_buf, dr_buf, gbuf, gpeer, gr0, gr1, gr2, gout, bsem, dsem, psem, ssem, rsem, own_sem = refs[20:]
    me, part = lax.axis_index("ep"), lax.axis_index("fsdp")
    n = xdy_ref.shape[0]
    meet_all(me, part)
    for ref in dws:
        ref[...] = jnp.zeros_like(ref)
    gather_weights(part, own, other, full)

    def block_copies(r):
        to = peer_at(me, r, -1)
        return [remote(buf.at[r], ref.at[me], sem, (r,), {"ep": to})
                for buf, ref, sem in ((dx_buf, back_ref, bsem), (dr_buf, dr_back, dsem))]

    keep = [pltpu.make_async_copy(buf.at[0], ref.at[me], own_sem.at[i])
            for i, (buf, ref) in enumerate(((dx_buf, back_ref), (dr_buf, dr_back)))]

    def fold_peer():
        gbuf[...] = gfull[part] + gpeer[...]

    phases = [(lambda: [remote(gfull.at[1 - part], gpeer, psem, (3,), {"fsdp": 1 - part})], fold_peer)]
    phases += all_reduce(me, gbuf, (gr0, gr1, gr2), lambda c, s: gout.at[c, s], ssem, rsem)

    def work(step):
        at = pl.ds(step * group, group)
        expert_body(depth, span, step, xdy_ref.at[at], rec_ref, *full, dx_buf.at[at], dr_buf.at[at], *dws)
        start_blocks(step, group, block_copies, keep)

    in_step(n // group, phases, work)

    size = LANES * 2
    here, there = (pl.ds(pl.multiple_of(p * size, LANES), size) for p in (part, 1 - part))
    swaps = [remote(dw.at[:, there, :] if i < 2 else dw.at[:, :, there], peer, psem, (i,), {"fsdp": 1 - part})
             for i, (dw, peer) in enumerate(zip(dws, peers))]
    for copy in swaps:
        copy.start()
    for copy in swaps:
        copy.wait()
    for i, (dw, peer, out) in enumerate(zip(dws, peers, outs)):
        rows, wide = out.shape[1:]
        for k in range(2):
            mine = top_ref[0:1, :] == 2 * me + k
            for b in range(wide // LANES):
                lanes = slice(b * LANES, (b + 1) * LANES)
                if i < 2:
                    total = dw[k, here, lanes]
                else:
                    total = dw[k, :, pl.ds(pl.multiple_of(part * size + b * LANES, LANES), LANES)]
                out[k, :, lanes] = total + peer[k, :, lanes] + only(mine, gout[i, b * rows:(b + 1) * rows, :])
    wait_blocks(n, block_copies, keep)


def dispatch_kernel(group, q_ref, x_ref, dy_ref, msg_ref, gate_ref, top_ref, wg_ref, wu_ref, wd_ref,
                    xdy_ref, rec_ref, dx_ref, dr_ref, gfull,
                    packed, rows_ref, wbuf, wr0, wr1, wr2, wfull, bsem, msem, psem, ssem, rsem, own_sem):
    me, part = lax.axis_index("ep"), lax.axis_index("fsdp")
    n_dest, rows, _ = xdy_ref.shape
    d = x_ref.shape[1]
    meet_all(me, part)

    def pack(slot):
        pick = hot((q_ref[0:1, :] == slot) | (q_ref[1:2, :] == slot))
        return nn(pick, x_ref[...]).astype(bf16), nn(pick, dy_ref[...]).astype(bf16)

    def block_copies(r):
        to = peer_at(me, r, 1)
        return [remote(packed.at[r], xdy_ref.at[r], bsem, (r,), {"ep": to}),
                remote(msg_ref.at[to], rec_ref.at[r], msem, (r,), {"ep": to})]

    keep = [pltpu.make_async_copy(packed.at[0], xdy_ref.at[0], own_sem.at[0]),
            pltpu.make_async_copy(msg_ref.at[me], rec_ref.at[0], own_sem.at[1])]

    def work(step):
        line = iota((group * rows, 1), 0)
        slot = line
        for j in range(group):
            inside = (line >= j * rows) & (line < (j + 1) * rows)
            slot = jnp.where(inside, line - j * rows + peer_at(me, step * group + j, 1) * rows, slot)
        x_rows, dy_rows = pack(slot)
        for j in range(group):
            at = slice(j * rows, (j + 1) * rows)
            packed[step * group + j, :, :d] = x_rows[at]
            packed[step * group + j, :, d:] = dy_rows[at]
        start_blocks(step, group, block_copies, keep)

    def serve_top():
        half, wide = d // 2, d // LANES
        mats = []
        for i in range(2):
            mats.append(jnp.concatenate([jnp.concatenate(
                [wfull[f, i, b * half:(b + 1) * half, :] for b in range(wide)], axis=1) for f in range(2)], axis=0))
        w2 = jnp.concatenate([wfull[f, 2, b * d:(b + 1) * d, :] for f in range(2) for b in range(wide // 2)], axis=1)
        n = rows_ref.shape[0]
        x = rows_ref[:, :d]
        dy = rows_ref[:, d:].astype(f32)
        eye = iota((n, n), 0) == iota((n, n), 1)
        weight = across(only(eye, gate_ref[0:1, :]))
        hidden, g, dh1, dh3, dx, dr = swiglu_rows(x, dy, weight, mats[0], mats[1], w2)
        dx_ref[...] = dx.astype(bf16)
        dr_ref[...] = jnp.broadcast_to(dr, dr_ref.shape)
        for i, dh in enumerate((dh1, dh3)):
            dw = tn(x, dh)
            for f in range(2):
                for b in range(wide):
                    gfull[f, i, b * half:(b + 1) * half, :] = dw[f * half:(f + 1) * half, b * LANES:(b + 1) * LANES]
        dw = tn(hidden, g)
        for f in range(2):
            for b in range(wide // 2):
                lane = f * half + b * LANES
                gfull[f, 2, b * d:(b + 1) * d, :] = dw[:, lane:lane + LANES]

    for i, w in enumerate((wg_ref, wu_ref, wd_ref)):
        n = w.shape[1]
        for b in range(w.shape[2] // LANES):
            lanes = slice(b * LANES, (b + 1) * LANES)
            mine = [only(top_ref[0:1, :] == 2 * me + k, w[k, :, lanes].astype(f32)) for k in range(2)]
            wbuf[i, b * n:(b + 1) * n, :] = (mine[0] + mine[1]).astype(bf16)
    phases = all_reduce(me, wbuf, (wr0, wr1, wr2), lambda c, s: wfull.at[part, c, s], ssem, rsem)
    phases += [(lambda: [remote(wfull.at[part], wfull.at[part], psem, (0,), {"fsdp": 1 - part})], serve_top)]
    x_rows, dy_rows = pack(iota((rows_ref.shape[0], 1), 0) + n_dest * rows)
    rows_ref[:, :d] = x_rows
    rows_ref[:, d:] = dy_rows
    in_step(n_dest // group, phases, work)
    wait_blocks(n_dest, block_copies, keep)


def dr_kernel(rows, span, ids_ref, q_ref, back_ref, *rest):
    top_dr_ref, out_ref = rest if len(rest) == 2 else (None, rest[0])
    n_src = back_ref.shape[0]
    tokens = ids_ref.shape[1]
    chunk = 512
    tables = split3(back_ref[...].T)
    for c in range(tokens // chunk):
        at = slice(c * chunk, (c + 1) * chunk)
        for j in range(2):
            block = ids_ref[j:j + 1, at] // 2
            q = q_ref[j:j + 1, at]
            owner = hot(iota((n_src, chunk), 0) == block)
            column = nn(tables[0], owner) + nn(tables[1], owner) + nn(tables[2], owner)
            far = q >= n_src * rows
            want = jnp.where(far, FAR, q - block * rows)
            picked = down(only(iota((span, chunk), 0) == want, column))
            if top_dr_ref is not None:
                want = jnp.where(far, q - n_src * rows, FAR)
                picked = picked + down(
                    only(iota((LANES, chunk), 0) == want, top_dr_ref[:, 0:1]))
            out_ref[j:j + 1, at] = picked


def combine_kernel(q_ref, back_ref, *rest):
    top_ref, out_ref = rest if len(rest) == 2 else (None, rest[0])
    rows, slots = q_ref.shape[0], back_ref.shape[0]
    q0, q1 = q_ref[:, 0:1], q_ref[:, 1:2]
    acc = jnp.zeros(out_ref.shape, f32)
    for at in range(0, slots, 512):
        depth = min(512, slots - at)
        column = iota((rows, depth), 1) + at
        pick = hot((q0 == column) | (q1 == column))
        acc = acc + nn(pick, back_ref[at:at + depth, :])
    if top_ref is not None:
        column = iota((rows, LANES), 1) + slots
        pick = hot((q0 == column) | (q1 == column))
        acc = acc + nn(pick, top_ref[...])
    out_ref[...] = acc.astype(bf16)


def vmem():
    return pl.BlockSpec(memory_space=pltpu.VMEM)


def whole(shape):
    return pl.BlockSpec(shape, lambda i: (0,) * len(shape))


PARAMS = pltpu.CompilerParams(vmem_limit_bytes=60 * 1024 * 1024)


def exchange(v):
    return lax.all_to_all(v, "ep", 0, 0, tiled=True)


ANYWHERE = pl.BlockSpec(memory_space=pl.ANY)


def reduce_scratch(dtype, total, n_mat=3):
    sizes = [total // SIDE ** (i + 1) for i in range(len(STRIDES))]
    sems = pltpu.SemaphoreType.DMA((2, len(STRIDES), n_mat, SIDE - 1))
    return [pltpu.VMEM((n_mat, SIDE - 1, size, LANES), dtype) for size in sizes], [sems, sems]


def comm_params(index):
    return pltpu.CompilerParams(vmem_limit_bytes=60 * 1024 * 1024, collective_id=index, has_side_effects=True)


def dispatch(q_t, x_tok, dy_tok, msg, gate, top, own, n_dest, rows):
    d, total = x_tok.shape[1], own[0].shape[1] * own[0].shape[2] // LANES
    part, both = (len(own), total, LANES), (2, len(own), total, LANES)
    recvs, sems = reduce_scratch(bf16, total)
    dma = pltpu.SemaphoreType.DMA
    return pl.pallas_call(
        functools.partial(dispatch_kernel, 8),
        out_shape=(jax.ShapeDtypeStruct((n_dest, rows, 2 * d), bf16),
                   jax.ShapeDtypeStruct(msg.shape, f32),
                   jax.ShapeDtypeStruct((LANES, d), bf16),
                   jax.ShapeDtypeStruct((LANES, LANES), f32),
                   jax.ShapeDtypeStruct(both, f32)),
        in_specs=[vmem()] * 9, out_specs=(ANYWHERE,) + (vmem(),) * 4,
        scratch_shapes=[pltpu.VMEM((n_dest, rows, 2 * d), bf16), pltpu.VMEM((LANES, 2 * d), bf16),
                        pltpu.VMEM(part, bf16), *recvs, pltpu.VMEM(both, bf16),
                        dma((2, n_dest)), dma((2, n_dest)), dma((2, 1)), *sems, dma((2,))],
        compiler_params=comm_params(0), name="dispatch",
    )(q_t, x_tok, dy_tok, msg, gate, top, *own)


class Plan:
    def __init__(self, rows, depth, pack_group, group, capacity, n_ep, local_top):
        self.rows, self.depth, self.pack_group, self.group = rows, depth, pack_group, group
        self.capacity, self.n_ep, self.local_top = capacity, n_ep, local_top
        self.span = -(-rows // LANES) * LANES

    def pack(self, q_t, x_tok, dy_tok, group, rows, steps):
        tok_dev, d = x_tok.shape
        return pl.pallas_call(
            pack_kernel,
            out_shape=jax.ShapeDtypeStruct((steps * group * rows, 2 * d), bf16),
            grid=(steps,),
            in_specs=[whole((2, tok_dev)), whole((tok_dev, d)), whole((tok_dev, d))],
            out_specs=pl.BlockSpec((group * rows, 2 * d), lambda i: (i, 0)),
            compiler_params=PARAMS, name="pack",
        )(q_t, x_tok, dy_tok)

    def route(self, ids_t, rw_t):
        n_ep, rows, span, tok_dev = self.n_ep, self.rows, self.span, ids_t.shape[1]
        q_t, _, msg, top, gate = pl.pallas_call(
            functools.partial(route_kernel, self.capacity, rows, self.depth, span, self.local_top),
            out_shape=(jax.ShapeDtypeStruct((2, tok_dev), i32), jax.ShapeDtypeStruct((2, tok_dev), i32),
                       jax.ShapeDtypeStruct((n_ep, 2 * span + LANES), f32),
                       jax.ShapeDtypeStruct((8, LANES), i32), jax.ShapeDtypeStruct((8, LANES), f32)),
            in_specs=[vmem(), vmem()], out_specs=(vmem(),) * 5, compiler_params=PARAMS, name="route",
        )(ids_t, rw_t)
        return q_t, msg, top, gate

    def forward(self, part, x_tok, dy_tok, ids_t, rw_t, weights, own):
        d = x_tok.shape[1]
        n_ep, rows = self.n_ep, self.rows
        q_t, msg, _, _ = self.route(ids_t, rw_t)
        rec = exchange(msg)
        packed = self.pack(q_t, x_tok, dy_tok, self.pack_group, rows, n_ep // self.pack_group)
        xdy = exchange(packed.reshape(n_ep, rows, 2 * d))
        dx, dr, *dws = self.experts(part, xdy, rec, weights, own)
        return q_t, exchange(dx), exchange(dr), dws

    def forward_top(self, x_tok, dy_tok, ids_t, rw_t, weights, own):
        n_ep, rows, span = self.n_ep, self.rows, self.span
        q_t, msg, top, gate = self.route(ids_t, rw_t)
        xdy, rec, top_dx, top_dr, top_grad = dispatch(
            q_t, x_tok, dy_tok, msg.reshape(n_ep, 1, -1), gate, top, own, n_ep, rows)
        rec = rec.reshape(n_ep, -1)
        back, dr, *grads = self.experts_send(xdy, rec, top, top_grad, weights, own)
        return rec[:, 2 * span:], top[0, 0], (q_t, back, dr, (top_dx, top_dr)), grads

    def experts(self, part, xdy, rec, weights, own):
        n_ep, rows, width = xdy.shape
        d, group, span = width // 2, self.group, self.span
        ff = own[0].shape[2]
        return pl.pallas_call(
            functools.partial(expert_kernel, self.depth, span),
            out_shape=(jax.ShapeDtypeStruct((n_ep, rows, d), bf16), jax.ShapeDtypeStruct((n_ep, 1, span), f32),
                       jax.ShapeDtypeStruct((2, d, ff), f32),
                       jax.ShapeDtypeStruct((2, d, ff), f32),
                       jax.ShapeDtypeStruct((2, ff, d), f32)),
            grid=(n_ep // group,),
            in_specs=[pl.BlockSpec(memory_space=pltpu.SMEM), pl.BlockSpec((group, rows, width), lambda i: (i, 0, 0)),
                      whole(rec.shape)] + [whole(w.shape) for w in (*own, *weights)],
            out_specs=(pl.BlockSpec((group, rows, d), lambda i: (i, 0, 0)),
                       pl.BlockSpec((group, 1, span), lambda i: (i, 0, 0)),
                       whole((2, d, ff)), whole((2, d, ff)), whole((2, ff, d))),
            scratch_shapes=[pltpu.VMEM((2, d, ff), bf16), pltpu.VMEM((2, d, ff), bf16), pltpu.VMEM((2, ff, d), bf16)],
            compiler_params=PARAMS, name="experts",
        )(part.reshape(1), xdy, rec, *own, *weights)

    def experts_send(self, xdy, rec, top, top_grad, weights, own):
        n_ep, rows, width = xdy.shape
        d, ff, span = width // 2, own[0].shape[2], self.span
        dma = pltpu.SemaphoreType.DMA
        full = [(2, d, ff), (2, d, ff), (2, ff, d)]
        part = top_grad.shape[1:]
        recvs, sems = reduce_scratch(f32, part[1])
        sum_refs = [pltpu.VMEM(part, f32), pltpu.VMEM(part, f32), *recvs, pltpu.VMEM(part, f32)]
        return pl.pallas_call(
            functools.partial(expert_send_kernel, self.depth, span, self.group),
            out_shape=(jax.ShapeDtypeStruct((n_ep, rows, d), bf16), jax.ShapeDtypeStruct((n_ep, 1, span), f32),
                       *(jax.ShapeDtypeStruct(w.shape, f32) for w in own)),
            in_specs=[vmem()] * 10, out_specs=(ANYWHERE,) + (vmem(),) * 4,
            scratch_shapes=[*(pltpu.VMEM(v, bf16) for v in full), *(pltpu.VMEM(v, f32) for v in full),
                            *(pltpu.VMEM(w.shape, f32) for w in own),
                            pltpu.VMEM((n_ep, rows, d), bf16), pltpu.VMEM((n_ep, 1, span), f32), *sum_refs,
                            dma((2, n_ep)), dma((2, n_ep)), dma((2, 4)), *sems, dma((2,))],
            compiler_params=comm_params(1), name="experts_send",
        )(xdy, rec, top, top_grad, *own, *weights)

    def finish(self, ids_t, q_t, back, dr, top_out):
        tok_dev, (n_ep, rows, d), tile = q_t.shape[1], back.shape, 256
        dr_args = [ids_t, q_t, dr.reshape(n_ep, -1)] + ([top_out[1]] if top_out else [])
        dr_t = pl.pallas_call(
            functools.partial(dr_kernel, self.rows, self.span), out_shape=jax.ShapeDtypeStruct((2, tok_dev), f32),
            in_specs=[vmem()] * len(dr_args), out_specs=vmem(), compiler_params=PARAMS, name="route_grad",
        )(*dr_args)
        args = [q_t.T, back.reshape(n_ep * rows, d)] + ([top_out[0]] if top_out else [])
        grad_x = pl.pallas_call(
            combine_kernel,
            out_shape=jax.ShapeDtypeStruct((tok_dev, d), bf16),
            grid=(tok_dev // tile,),
            in_specs=[pl.BlockSpec((tile, 2), lambda i: (i, 0))] + [whole(v.shape) for v in args[1:]],
            out_specs=pl.BlockSpec((tile, d), lambda i: (i, 0)),
            compiler_params=PARAMS, name="combine",
        )(*args)
        return grad_x, dr_t.T


def solution(mesh):
    n_ep = mesh.shape["ep"]
    tok_spec = P(("fsdp", "ep"), None)
    spec_in = P("ep", "fsdp", None)
    spec_out = P("ep", None, "fsdp")

    def per_device(x_tok, dy_tok, expert_ids, route_w, w_gate, w_up, w_down):
        tok_dev, top_k = expert_ids.shape
        capacity = capacity_of(tok_dev, top_k, w_gate.shape[0] * n_ep)
        part = lax.axis_index("fsdp").astype(i32)
        swap = [(0, 1), (1, 0)]
        own = (w_gate, w_up, w_down)
        weights = [lax.ppermute(w, "fsdp", swap) for w in own]
        ids_t = expert_ids.T
        inputs = (x_tok, dy_tok, ids_t, route_w.T, weights, own)

        def shard_halves(dws):
            out = []
            for dw, axis in zip(dws, (1, 1, 2)):
                size = dw.shape[axis] // 2
                keep = lax.dynamic_slice_in_dim(dw, part * size, size, axis)
                give = lax.dynamic_slice_in_dim(dw, (1 - part) * size, size, axis)
                out.append(keep + lax.ppermute(give, "fsdp", swap))
            return out

        quick = Plan(72, 48, 4, 8, capacity, n_ep, True)
        safe = Plan(2 * capacity, capacity, 2, 4, capacity, n_ep, False)
        notes, top_id, mine, grads = quick.forward_top(*inputs)
        agree = jnp.all(notes[:, 1] == top_id.astype(f32)) & jnp.all(notes[:, 0] == 0.0)
        note = jnp.where(agree, top_id.astype(f32), -1.0).reshape(1, 1)
        other = lax.ppermute(note, "fsdp", swap)
        good = agree & (other == note)[0, 0]

        def fits():
            return (*quick.finish(ids_t, *mine), *grads)

        def general():
            q_all, back_all, dr_all, dws = safe.forward(part, *inputs)
            return (*safe.finish(ids_t, q_all, back_all, dr_all, None), *shard_halves(dws))

        return lax.cond(good, fits, general)

    return jax.shard_map(
        per_device, mesh=mesh,
        in_specs=(tok_spec, tok_spec, tok_spec, tok_spec, spec_in, spec_in, spec_out),
        out_specs=(tok_spec, tok_spec, spec_in, spec_in, spec_out),
        check_vma=False)
```

```python
import functools

import jax
import jax.numpy as jnp
from jax import lax
from jax.experimental import pallas as pl
from jax.experimental.pallas import tpu as pltpu
from jax.sharding import PartitionSpec as P

CAP_FACTOR = 3
LANES = 128
FAR = 1 << 20
MESH = pl.DeviceIdType.MESH
LAG = 2
f32, bf16, i32 = jnp.float32, jnp.bfloat16, jnp.int32


def capacity_of(tok_dev, top_k, experts):
    return max(8, ((CAP_FACTOR * tok_dev * top_k // experts + 7) // 8) * 8)


def iota(shape, dim):
    return lax.broadcasted_iota(i32, shape, dim)


def nn(a, b):
    return jnp.dot(a, b, preferred_element_type=f32)


def nt(a, b):
    return lax.dot_general(a, b, (((1,), (1,)), ((), ())), preferred_element_type=f32)


def tn(a, b):
    return lax.dot_general(a, b, (((0,), (0,)), ((), ())), preferred_element_type=f32)


def split3(v):
    hi = v.astype(bf16)
    rest = v - hi.astype(f32)
    mid = rest.astype(bf16)
    lo = (rest - mid.astype(f32)).astype(bf16)
    return hi, mid, lo


def hot(mask):
    return jnp.where(mask, 1.0, 0.0).astype(bf16)


def only(mask, v):
    return jnp.where(mask, v, jnp.zeros_like(v))


def down(v):
    return jnp.sum(v, axis=0, keepdims=True)


def across(v):
    return jnp.sum(v, axis=1, keepdims=True)


def add3(v, n):
    return v[:, :n] + v[:, n:2 * n] + v[:, 2 * n:]


SIDE = 4
STRIDES = (1, SIDE, SIDE * SIDE)


def coords(me):
    return [me % SIDE, (me // SIDE) % SIDE, me // (SIDE * SIDE)]


def peer_at(me, r, sign):
    o = (r * 23) % SIDE ** 3
    out = 0
    for here, off, stride in zip(coords(me), coords(o)[::-1], STRIDES):
        out = out + ((here + sign * off + SIDE) % SIDE) * stride
    return out


def meet_all(me, part):
    barrier = pltpu.get_barrier_semaphore()
    n = SIDE ** 3

    @pl.loop(1, n)
    def _(r):
        pl.semaphore_signal(barrier, inc=1, device_id={"ep": peer_at(me, r, 1)}, device_id_type=MESH)

    pl.semaphore_signal(barrier, inc=1, device_id={"fsdp": 1 - part}, device_id_type=MESH)
    pl.semaphore_wait(barrier, n)


def remote(src, dst, sems, at, to, back=None):
    return pltpu.make_async_remote_copy(
        src_ref=src, dst_ref=dst, send_sem=sems.at[(0, *at)], recv_sem=sems.at[(1, *(back or at))],
        device_id=to, device_id_type=MESH)


def start_blocks(step, group, copies, keep):
    for j in range(group):
        if j == 0:
            @pl.when(step == 0)
            def _():
                for copy in keep:
                    copy.start()

            @pl.when(step > 0)
            def _():
                for copy in copies(step * group):
                    copy.start()
        else:
            for copy in copies(step * group + j):
                copy.start()


def wait_blocks(n, copies, keep):
    for copy in keep:
        copy.wait()

    @pl.loop(1, n)
    def _(r):
        for copy in copies(r):
            copy.wait()


def in_step(steps, phases, work):
    @pl.loop(0, max(steps, len(phases)))
    def _(step):
        for i, (copies, _) in enumerate(phases):
            @pl.when(step == i)
            def _(copies=copies):
                for copy in copies():
                    copy.start()

        @pl.when(step < steps)
        def _():
            work(step)

        for i, (copies, then) in enumerate(phases):
            @pl.when(step == i)
            def _(copies=copies, then=then):
                for copy in copies():
                    copy.wait()
                if then is not None:
                    then()


def all_reduce(me, buf, recvs, put, sems_out, sems_in):
    coord = coords(me)
    n_mat, total = buf.shape[0], buf.shape[1]
    levels = len(STRIDES)
    sizes = [total // SIDE ** (level + 1) for level in range(levels)]

    def at(base, size):
        return pl.ds(pl.multiple_of(base, 16), size)

    def base_of(c, level):
        base = 0
        for i in range(level):
            base = base + coord[(c + i) % levels] * sizes[i]
        return base

    def lines(level):
        for c in range(n_mat):
            axis = (c + level) % levels
            for delta in range(1, SIDE):
                to = (coord[axis] + delta) % SIDE
                yield c, delta, to, {"ep": me + (to - coord[axis]) * STRIDES[axis]}

    def scatter(level):
        return [remote(buf.at[c, at(base_of(c, level) + to * sizes[level], sizes[level])], recvs[level].at[c, 3 - delta],
                       sems_out, (level, c, delta - 1), peer, (level, c, 3 - delta))
                for c, delta, to, peer in lines(level)]

    def gather(level):
        out = []
        for c, delta, _, peer in lines(level):
            mine = put(c, at(base_of(c, level + 1), sizes[level]))
            out.append(remote(mine, mine, sems_in, (level, c, delta - 1), peer, (level, c, 3 - delta)))
        return out

    def add(level):
        for c in range(n_mat):
            mine = at(base_of(c, level + 1), sizes[level])
            value = buf[c, mine].astype(f32)
            for i in range(SIDE - 1):
                value = value + recvs[level][c, i].astype(f32)
            if level == levels - 1:
                put(c, mine)[...] = value.astype(buf.dtype)
            else:
                buf[c, mine] = value.astype(buf.dtype)

    return ([(functools.partial(scatter, level), functools.partial(add, level)) for level in range(levels)]
            + [(functools.partial(gather, level), None) for level in reversed(range(levels))])


def route_kernel(capacity, rows, depth, span, local_top, ids_ref, rw_ref, q_ref, pos_ref, msg_ref, top_ref, topw_ref):
    experts, chunk = LANES, 256
    tokens = ids_ref.shape[1]
    n_dest = msg_ref.shape[0]
    before = (iota((chunk, chunk), 0) < iota((chunk, chunk), 1)).astype(bf16)
    expert_id = iota((experts, chunk), 0)
    slot_id = iota((span, chunk), 0)
    half_id = iota((n_dest, chunk), 0) * 2
    seen = jnp.zeros((experts, 1), f32)
    for c in range(tokens // chunk):
        at = slice(c * chunk, (c + 1) * chunk)
        hits = [expert_id == ids_ref[j:j + 1, at] for j in range(2)]
        member = jnp.where(hits[0] | hits[1], 1.0, 0.0)
        earlier = nn(member.astype(bf16), before) + seen
        seen = seen + across(member)
        for j in range(2):
            pos_ref[j:j + 1, at] = down(only(hits[j], earlier)).astype(i32)
    expert_col = iota((experts, 1), 0).astype(f32)
    kept = jnp.minimum(seen, float(capacity))
    if local_top:
        most = jnp.max(seen, axis=0, keepdims=True)
        top = jnp.min(jnp.where(seen == most, expert_col, float(experts)), axis=0, keepdims=True)
        kept = jnp.where(expert_col == top, 0.0, kept)
    else:
        top = jnp.full((1, 1), -1.0, f32)
    top_i = top.astype(i32)
    gates = [jnp.zeros((3 * n_dest, span), f32) for _ in range(2)]
    top_gates = jnp.zeros((24, LANES), f32)
    for c in range(tokens // chunk):
        at = slice(c * chunk, (c + 1) * chunk)
        for j in range(2):
            ids = ids_ref[j:j + 1, at]
            place = pos_ref[j:j + 1, at]
            weight = rw_ref[j:j + 1, at]
            keep = place < capacity
            slot = jnp.where(ids % 2 == 0, place, rows - 1 - place)
            q = (ids // 2) * rows + slot
            if local_top:
                is_top = ids == top_i
                q = jnp.where(is_top, n_dest * rows + place, q)
                slot = jnp.where(is_top, FAR, slot)
                top_hot = hot((iota((LANES, chunk), 0) == place) & keep & is_top)
                top_parts = [jnp.broadcast_to(p, (8, chunk)) for p in split3(weight)]
                top_gates = top_gates + nt(jnp.concatenate(top_parts, axis=0), top_hot)
            q_ref[j:j + 1, at] = jnp.where(keep, q, FAR)
            slot_hot = hot(slot_id == jnp.where(keep, slot, FAR))
            for par in range(2):
                mine = only(half_id + par == ids, weight)
                gates[par] = gates[par] + nt(jnp.concatenate(split3(mine), axis=0), slot_hot)
    kept_wide = jnp.broadcast_to(kept, (experts, LANES)).astype(bf16)
    owner = (iota((n_dest, experts), 1) // 2 == iota((n_dest, experts), 0)).astype(bf16)
    over = jnp.max(jnp.where(nn(owner, kept_wide) > float(rows), 1.0, 0.0), axis=0, keepdims=True)
    over = jnp.maximum(over, jnp.max(jnp.where(kept > float(depth), 1.0, 0.0), axis=0, keepdims=True))
    for par in range(2):
        g = gates[par]
        msg_ref[:, 0, par * span:(par + 1) * span] = g[:n_dest] + g[n_dest:2 * n_dest] + g[2 * n_dest:]
    note = jnp.where(iota((1, LANES), 1) == 1, top, over)
    msg_ref[:, 0, 2 * span:] = jnp.broadcast_to(note, (n_dest, LANES))
    top_ref[...] = jnp.broadcast_to(top_i, (8, LANES))
    topw_ref[...] = top_gates[:8] + top_gates[8:16] + top_gates[16:]


def pack_kernel(q_ref, x_ref, dy_ref, out_ref):
    d, count = x_ref.shape[1], out_ref.shape[0]
    slot = iota((count, 1), 0) + pl.program_id(0) * count
    pick = hot((q_ref[0:1, :] == slot) | (q_ref[1:2, :] == slot))
    out_ref[:, :d] = nn(pick, x_ref[...]).astype(bf16)
    out_ref[:, d:] = nn(pick, dy_ref[...]).astype(bf16)


def swiglu_rows(x, dy, weight, w1, w3, w2):
    h1 = nn(x, w1)
    h3 = nn(x, w3)
    s = jax.nn.sigmoid(h1)
    hidden = (h1 * s * h3).astype(bf16)
    dr = across(dy * nn(hidden, w2))
    g = (weight * dy).astype(bf16)
    da = nt(g, w2)
    dh1 = (da * h3 * s * (1.0 + h1 * (1.0 - s))).astype(bf16)
    dh3 = (da * h1 * s).astype(bf16)
    return hidden, g, dh1, dh3, nt(dh1, w1) + nt(dh3, w3), dr


def expert_body(depth, span, step, xdy_ref, rec_ref, w1_ref, w3_ref, w2_ref, dx_ref, dr_ref, dwg_ref, dwu_ref, dwd_ref):
    group, rows, width = xdy_ref.shape
    n_src = rec_ref.shape[0]
    d = width // 2
    m = group * depth

    local = iota((m, n_src), 0) // depth
    src_hot = hot(local + step * group == iota((m, n_src), 1))
    row_hot = hot(iota((m, LANES), 0) // depth == iota((m, LANES), 1))
    within = iota((m, span), 0) % depth
    outs, dr_slots = [], jnp.zeros((LANES, span), f32)
    for k in range(2):
        first = 0 if k == 0 else rows - depth
        slot_hot = iota((m, span), 1) == within + first
        gate_parts = jnp.concatenate(split3(rec_ref[:, k * span:(k + 1) * span]), axis=1)
        weight = across(only(slot_hot, add3(nn(src_hot, gate_parts), span)))
        x = xdy_ref[:, first:first + depth, :d].reshape(m, d)
        dy = xdy_ref[:, first:first + depth, d:].reshape(m, d).astype(f32)
        hidden, g, dh1, dh3, dx, dr = swiglu_rows(x, dy, weight, w1_ref[k], w3_ref[k], w2_ref[k])
        outs.append(dx.reshape(group, depth, d))
        dwg_ref[k] += tn(x, dh1)
        dwu_ref[k] += tn(x, dh3)
        dwd_ref[k] += tn(hidden, g)
        parts = jnp.concatenate(split3(only(slot_hot & (weight > 0.0), dr)), axis=1)
        dr_slots = dr_slots + add3(tn(row_hot, parts), span)
    low = rows - depth
    dx_ref[:, :low] = outs[0][:, :low].astype(bf16)
    if depth > low:
        dx_ref[:, low:depth] = (outs[0][:, low:] + outs[1][:, :depth - low]).astype(bf16)
    dx_ref[:, depth:] = outs[1][:, depth - low:].astype(bf16)
    for i in range(group):
        dr_ref[i] = dr_slots[i:i + 1]


def gather_weights(part, own, other, full):
    for mine, theirs, whole_ref, by_rows in zip(own, other, full, (True, True, False)):
        size = mine.shape[1] if by_rows else mine.shape[2]
        for ref, at in ((mine, part * size), (theirs, (1 - part) * size)):
            at = pl.ds(pl.multiple_of(at, LANES), size)
            for k in range(2):
                if by_rows:
                    whole_ref[k, at, :] = ref[k]
                else:
                    whole_ref[k, :, at] = ref[k]


def expert_kernel(depth, span, part_ref, xdy_ref, rec_ref, *refs):
    own, other, (dx_ref, dr_ref), dws, full = refs[:3], refs[3:6], refs[6:8], refs[8:11], refs[11:]
    step = pl.program_id(0)

    @pl.when(step == 0)
    def _():
        for ref in dws:
            ref[...] = jnp.zeros_like(ref)
        gather_weights(part_ref[0], own, other, full)

    expert_body(depth, span, step, xdy_ref, rec_ref, *full, dx_ref, dr_ref, *dws)


def expert_send_kernel(depth, span, group, q_ref, top_dx_ref, xdy_ref, rec_ref, top_ref, gfull, *refs):
    own, other, gx_ref, dr_back, outs = refs[:3], refs[3:6], refs[6], refs[7], refs[8:11]
    full, dws, peers = refs[11:14], refs[14:17], refs[17:20]
    back_ref, acc_ref, dx_buf, dr_buf, gbuf, gpeer, gr0, gr1, gr2, gout, bsem, dsem, psem, ssem, rsem, own_sem = refs[20:]
    me, part = lax.axis_index("ep"), lax.axis_index("fsdp")
    n = xdy_ref.shape[0]
    meet_all(me, part)
    for ref in dws:
        ref[...] = jnp.zeros_like(ref)
    gather_weights(part, own, other, full)

    def block_copies(r):
        to = peer_at(me, r, -1)
        return [remote(dx_buf.at[r], back_ref.at[r], bsem, (r,), {"ep": to}),
                remote(dr_buf.at[r], dr_back.at[me], dsem, (r,), {"ep": to})]

    keep = [pltpu.make_async_copy(dx_buf.at[0], back_ref.at[0], own_sem.at[0]),
            pltpu.make_async_copy(dr_buf.at[0], dr_back.at[me], own_sem.at[1])]

    def fold_peer():
        gbuf[...] = gfull[part] + gpeer[...]

    phases = [(lambda: [remote(gfull.at[1 - part], gpeer, psem, (3,), {"fsdp": 1 - part})], fold_peer)]
    phases += all_reduce(me, gbuf, (gr0, gr1, gr2), lambda c, s: gout.at[c, s], ssem, rsem)

    rows, tile = xdy_ref.shape[1], LANES * 2

    def combine(slot, block, fresh):
        @pl.loop(0, gx_ref.shape[0] // tile)
        def _(i):
            at = pl.ds(pl.multiple_of(i * tile, tile), tile)
            q = q_ref[at, :]
            value = nn(hot((q[:, 0:1] == slot) | (q[:, 1:2] == slot)), block)
            acc_ref[at, :] = value if fresh else acc_ref[at, :] + value

    def take(step):
        for j in range(group):
            r = step * group + j
            if j > 0:
                copies = block_copies(r)
                for copy in copies:
                    copy.wait()
            else:
                @pl.when(step == 0)
                def _():
                    for copy in keep:
                        copy.wait()

                @pl.when(step > 0)
                def _(r=r):
                    for copy in block_copies(r):
                        copy.wait()
        line = iota((1, group * rows), 1)
        slot = line
        for j in range(group):
            inside = (line >= j * rows) & (line < (j + 1) * rows)
            slot = jnp.where(inside, line - j * rows + peer_at(me, step * group + j, 1) * rows, slot)
        block = jnp.concatenate([back_ref[step * group + j].astype(f32) for j in range(group)], axis=0)
        combine(slot, block.astype(bf16), False)

    def work(step):
        at = pl.ds(step * group, group)
        expert_body(depth, span, step, xdy_ref.at[at], rec_ref, *full, dx_buf.at[at], dr_buf.at[at], *dws)
        start_blocks(step, group, block_copies, keep)

        @pl.when(step == 0)
        def _():
            combine(iota((1, LANES), 1) + n * rows, top_dx_ref[...], True)

        @pl.when(step >= LAG)
        def _():
            take(step - LAG)

    in_step(n // group, phases, work)

    size = LANES * 2
    here, there = (pl.ds(pl.multiple_of(p * size, LANES), size) for p in (part, 1 - part))
    swaps = [remote(dw.at[:, there, :] if i < 2 else dw.at[:, :, there], peer, psem, (i,), {"fsdp": 1 - part})
             for i, (dw, peer) in enumerate(zip(dws, peers))]
    for copy in swaps:
        copy.start()
    for step in range(n // group - LAG, n // group):
        take(step)
    gx_ref[...] = acc_ref[...].astype(bf16)
    for copy in swaps:
        copy.wait()
    for i, (dw, peer, out) in enumerate(zip(dws, peers, outs)):
        rows, wide = out.shape[1:]
        for k in range(2):
            mine = top_ref[0:1, :] == 2 * me + k
            for b in range(wide // LANES):
                lanes = slice(b * LANES, (b + 1) * LANES)
                if i < 2:
                    total = dw[k, here, lanes]
                else:
                    total = dw[k, :, pl.ds(pl.multiple_of(part * size + b * LANES, LANES), LANES)]
                out[k, :, lanes] = total + peer[k, :, lanes] + only(mine, gout[i, b * rows:(b + 1) * rows, :])


def dispatch_kernel(group, q_ref, x_ref, dy_ref, msg_ref, gate_ref, top_ref, wg_ref, wu_ref, wd_ref,
                    xdy_ref, rec_ref, dx_ref, dr_ref, gfull,
                    packed, wbuf, wr0, wr1, wr2, wfull, bsem, msem, psem, ssem, rsem, own_sem):
    me, part = lax.axis_index("ep"), lax.axis_index("fsdp")
    n_dest, rows, _ = xdy_ref.shape
    d = x_ref.shape[1]
    meet_all(me, part)

    def pack(slot):
        pick = hot((q_ref[0:1, :] == slot) | (q_ref[1:2, :] == slot))
        return nn(pick, x_ref[...]).astype(bf16), nn(pick, dy_ref[...]).astype(bf16)

    def block_copies(r):
        to = peer_at(me, r, 1)
        return [remote(packed.at[r], xdy_ref.at[r], bsem, (r,), {"ep": to}),
                remote(msg_ref.at[to], rec_ref.at[r], msem, (r,), {"ep": to})]

    keep = [pltpu.make_async_copy(packed.at[0], xdy_ref.at[0], own_sem.at[0]),
            pltpu.make_async_copy(msg_ref.at[me], rec_ref.at[0], own_sem.at[1])]

    def work(step):
        line = iota((group * rows, 1), 0)
        slot = line
        for j in range(group):
            inside = (line >= j * rows) & (line < (j + 1) * rows)
            slot = jnp.where(inside, line - j * rows + peer_at(me, step * group + j, 1) * rows, slot)
        x_rows, dy_rows = pack(slot)
        for j in range(group):
            at = slice(j * rows, (j + 1) * rows)
            packed[step * group + j, :, :d] = x_rows[at]
            packed[step * group + j, :, d:] = dy_rows[at]
        start_blocks(step, group, block_copies, keep)

    def serve_top():
        half, wide = d // 2, d // LANES
        mats = []
        for i in range(2):
            mats.append(jnp.concatenate([jnp.concatenate(
                [wfull[f, i, b * half:(b + 1) * half, :] for b in range(wide)], axis=1) for f in range(2)], axis=0))
        w2 = jnp.concatenate([wfull[f, 2, b * d:(b + 1) * d, :] for f in range(2) for b in range(wide // 2)], axis=1)
        n = dx_ref.shape[0]
        x, dy = pack(iota((n, 1), 0) + n_dest * rows)
        dy = dy.astype(f32)
        eye = iota((n, n), 0) == iota((n, n), 1)
        weight = across(only(eye, gate_ref[0:1, :]))
        hidden, g, dh1, dh3, dx, dr = swiglu_rows(x, dy, weight, mats[0], mats[1], w2)
        dx_ref[...] = dx.astype(bf16)
        dr_ref[...] = jnp.broadcast_to(dr, dr_ref.shape)
        for i, dh in enumerate((dh1, dh3)):
            dw = tn(x, dh)
            for f in range(2):
                for b in range(wide):
                    gfull[f, i, b * half:(b + 1) * half, :] = dw[f * half:(f + 1) * half, b * LANES:(b + 1) * LANES]
        dw = tn(hidden, g)
        for f in range(2):
            for b in range(wide // 2):
                lane = f * half + b * LANES
                gfull[f, 2, b * d:(b + 1) * d, :] = dw[:, lane:lane + LANES]

    for i, w in enumerate((wg_ref, wu_ref, wd_ref)):
        n = w.shape[1]
        for b in range(w.shape[2] // LANES):
            lanes = slice(b * LANES, (b + 1) * LANES)
            mine = [only(top_ref[0:1, :] == 2 * me + k, w[k, :, lanes].astype(f32)) for k in range(2)]
            wbuf[i, b * n:(b + 1) * n, :] = (mine[0] + mine[1]).astype(bf16)
    phases = all_reduce(me, wbuf, (wr0, wr1, wr2), lambda c, s: wfull.at[part, c, s], ssem, rsem)
    phases += [(lambda: [remote(wfull.at[part], wfull.at[part], psem, (0,), {"fsdp": 1 - part})], serve_top)]
    in_step(n_dest // group, phases, work)
    wait_blocks(n_dest, block_copies, keep)


def dr_kernel(rows, span, ids_ref, q_ref, back_ref, *rest):
    top_dr_ref, out_ref = rest if len(rest) == 2 else (None, rest[0])
    n_src = back_ref.shape[0]
    tokens = ids_ref.shape[1]
    chunk = 512
    tables = split3(back_ref[...].T)
    for c in range(tokens // chunk):
        at = slice(c * chunk, (c + 1) * chunk)
        for j in range(2):
            block = ids_ref[j:j + 1, at] // 2
            q = q_ref[j:j + 1, at]
            owner = hot(iota((n_src, chunk), 0) == block)
            column = nn(tables[0], owner) + nn(tables[1], owner) + nn(tables[2], owner)
            far = q >= n_src * rows
            want = jnp.where(far, FAR, q - block * rows)
            picked = down(only(iota((span, chunk), 0) == want, column))
            if top_dr_ref is not None:
                want = jnp.where(far, q - n_src * rows, FAR)
                picked = picked + down(
                    only(iota((LANES, chunk), 0) == want, top_dr_ref[:, 0:1]))
            out_ref[j:j + 1, at] = picked


def combine_kernel(q_ref, back_ref, out_ref):
    rows, slots = q_ref.shape[0], back_ref.shape[0]
    q0, q1 = q_ref[:, 0:1], q_ref[:, 1:2]
    depth = 512

    def body(i, acc):
        at = i * depth
        column = iota((rows, depth), 1) + at
        return acc + nn(hot((q0 == column) | (q1 == column)), back_ref[pl.ds(pl.multiple_of(at, depth), depth), :])

    out_ref[...] = lax.fori_loop(0, slots // depth, body, jnp.zeros(out_ref.shape, f32)).astype(bf16)


def vmem():
    return pl.BlockSpec(memory_space=pltpu.VMEM)


def whole(shape):
    return pl.BlockSpec(shape, lambda i: (0,) * len(shape))


PARAMS = pltpu.CompilerParams(vmem_limit_bytes=60 * 1024 * 1024)


def exchange(v):
    return lax.all_to_all(v, "ep", 0, 0, tiled=True)


ANYWHERE = pl.BlockSpec(memory_space=pl.ANY)


def reduce_scratch(dtype, total, n_mat=3):
    sizes = [total // SIDE ** (i + 1) for i in range(len(STRIDES))]
    sems = pltpu.SemaphoreType.DMA((2, len(STRIDES), n_mat, SIDE - 1))
    return [pltpu.VMEM((n_mat, SIDE - 1, size, LANES), dtype) for size in sizes], [sems, sems]


def comm_params(index):
    return pltpu.CompilerParams(vmem_limit_bytes=63 * 1024 * 1024, collective_id=index, has_side_effects=True)


def dispatch(q_t, x_tok, dy_tok, msg, gate, top, own, n_dest, rows):
    d, total = x_tok.shape[1], own[0].shape[1] * own[0].shape[2] // LANES
    part, both = (len(own), total, LANES), (2, len(own), total, LANES)
    recvs, sems = reduce_scratch(bf16, total)
    dma = pltpu.SemaphoreType.DMA
    return pl.pallas_call(
        functools.partial(dispatch_kernel, 8),
        out_shape=(jax.ShapeDtypeStruct((n_dest, rows, 2 * d), bf16),
                   jax.ShapeDtypeStruct(msg.shape, f32),
                   jax.ShapeDtypeStruct((LANES, d), bf16),
                   jax.ShapeDtypeStruct((LANES, LANES), f32),
                   jax.ShapeDtypeStruct(both, f32)),
        in_specs=[vmem()] * 9, out_specs=(ANYWHERE,) + (vmem(),) * 4,
        scratch_shapes=[pltpu.VMEM((n_dest, rows, 2 * d), bf16),
                        pltpu.VMEM(part, bf16), *recvs, pltpu.VMEM(both, bf16),
                        dma((2, n_dest)), dma((2, n_dest)), dma((2, 1)), *sems, dma((2,))],
        compiler_params=comm_params(0), name="dispatch",
    )(q_t, x_tok, dy_tok, msg, gate, top, *own)


class Plan:
    def __init__(self, rows, depth, pack_group, group, capacity, n_ep, local_top):
        self.rows, self.depth, self.pack_group, self.group = rows, depth, pack_group, group
        self.capacity, self.n_ep, self.local_top = capacity, n_ep, local_top
        self.span = -(-rows // LANES) * LANES

    def pack(self, q_t, x_tok, dy_tok, group, rows, steps):
        tok_dev, d = x_tok.shape
        return pl.pallas_call(
            pack_kernel,
            out_shape=jax.ShapeDtypeStruct((steps * group * rows, 2 * d), bf16),
            grid=(steps,),
            in_specs=[whole((2, tok_dev)), whole((tok_dev, d)), whole((tok_dev, d))],
            out_specs=pl.BlockSpec((group * rows, 2 * d), lambda i: (i, 0)),
            compiler_params=PARAMS, name="pack",
        )(q_t, x_tok, dy_tok)

    def route(self, ids_t, rw_t):
        n_ep, rows, span, tok_dev = self.n_ep, self.rows, self.span, ids_t.shape[1]
        q_t, _, msg, top, gate = pl.pallas_call(
            functools.partial(route_kernel, self.capacity, rows, self.depth, span, self.local_top),
            out_shape=(jax.ShapeDtypeStruct((2, tok_dev), i32), jax.ShapeDtypeStruct((2, tok_dev), i32),
                       jax.ShapeDtypeStruct((n_ep, 1, 2 * span + LANES), f32),
                       jax.ShapeDtypeStruct((8, LANES), i32), jax.ShapeDtypeStruct((8, LANES), f32)),
            in_specs=[vmem(), vmem()], out_specs=(vmem(),) * 5, compiler_params=PARAMS, name="route",
        )(ids_t, rw_t)
        return q_t, msg, top, gate

    def forward(self, part, x_tok, dy_tok, ids_t, rw_t, weights, own):
        d = x_tok.shape[1]
        n_ep, rows = self.n_ep, self.rows
        q_t, msg, _, _ = self.route(ids_t, rw_t)
        rec = exchange(msg).reshape(n_ep, -1)
        packed = self.pack(q_t, x_tok, dy_tok, self.pack_group, rows, n_ep // self.pack_group)
        xdy = exchange(packed.reshape(n_ep, rows, 2 * d))
        dx, dr, *dws = self.experts(part, xdy, rec, weights, own)
        return q_t, exchange(dx), exchange(dr), dws

    def forward_top(self, x_tok, dy_tok, ids_t, rw_t, weights, own):
        n_ep, rows, span = self.n_ep, self.rows, self.span
        q_t, msg, top, gate = self.route(ids_t, rw_t)
        xdy, rec, top_dx, top_dr, top_grad = dispatch(
            q_t, x_tok, dy_tok, msg, gate, top, own, n_ep, rows)
        rec = rec.reshape(n_ep, -1)
        grad_x, dr, *grads = self.experts_send(q_t, top_dx, xdy, rec, top, top_grad, weights, own)
        return rec[:, 2 * span:], top[0, 0], (q_t, dr, top_dr), grad_x, grads

    def experts(self, part, xdy, rec, weights, own):
        n_ep, rows, width = xdy.shape
        d, group, span = width // 2, self.group, self.span
        ff = own[0].shape[2]
        return pl.pallas_call(
            functools.partial(expert_kernel, self.depth, span),
            out_shape=(jax.ShapeDtypeStruct((n_ep, rows, d), bf16), jax.ShapeDtypeStruct((n_ep, 1, span), f32),
                       jax.ShapeDtypeStruct((2, d, ff), f32),
                       jax.ShapeDtypeStruct((2, d, ff), f32),
                       jax.ShapeDtypeStruct((2, ff, d), f32)),
            grid=(n_ep // group,),
            in_specs=[pl.BlockSpec(memory_space=pltpu.SMEM), pl.BlockSpec((group, rows, width), lambda i: (i, 0, 0)),
                      whole(rec.shape)] + [whole(w.shape) for w in (*own, *weights)],
            out_specs=(pl.BlockSpec((group, rows, d), lambda i: (i, 0, 0)),
                       pl.BlockSpec((group, 1, span), lambda i: (i, 0, 0)),
                       whole((2, d, ff)), whole((2, d, ff)), whole((2, ff, d))),
            scratch_shapes=[pltpu.VMEM((2, d, ff), bf16), pltpu.VMEM((2, d, ff), bf16), pltpu.VMEM((2, ff, d), bf16)],
            compiler_params=PARAMS, name="experts",
        )(part.reshape(1), xdy, rec, *own, *weights)

    def experts_send(self, q_t, top_dx, xdy, rec, top, top_grad, weights, own):
        n_ep, rows, width = xdy.shape
        d, ff, span = width // 2, own[0].shape[2], self.span
        dma = pltpu.SemaphoreType.DMA
        full = [(2, d, ff), (2, d, ff), (2, ff, d)]
        part = top_grad.shape[1:]
        recvs, sems = reduce_scratch(f32, part[1])
        sum_refs = [pltpu.VMEM(part, f32), pltpu.VMEM(part, f32), *recvs, pltpu.VMEM(part, f32)]
        return pl.pallas_call(
            functools.partial(expert_send_kernel, self.depth, span, self.group),
            out_shape=(jax.ShapeDtypeStruct((q_t.shape[1], d), bf16), jax.ShapeDtypeStruct((n_ep, 1, span), f32),
                       *(jax.ShapeDtypeStruct(w.shape, f32) for w in own)),
            in_specs=[vmem()] * 12, out_specs=(vmem(),) * 5,
            scratch_shapes=[*(pltpu.VMEM(v, bf16) for v in full), *(pltpu.VMEM(v, f32) for v in full),
                            *(pltpu.VMEM(w.shape, f32) for w in own),
                            pltpu.VMEM((n_ep, rows, d), bf16), pltpu.VMEM((q_t.shape[1], d), f32),
                            pltpu.VMEM((n_ep, rows, d), bf16), pltpu.VMEM((n_ep, 1, span), f32), *sum_refs,
                            dma((2, n_ep)), dma((2, n_ep)), dma((2, 4)), *sems, dma((2,))],
            compiler_params=comm_params(1), name="experts_send",
        )(q_t.T, top_dx, xdy, rec, top, top_grad, *own, *weights)

    def route_grad(self, ids_t, q_t, dr, *top_dr):
        return pl.pallas_call(
            functools.partial(dr_kernel, self.rows, self.span), out_shape=jax.ShapeDtypeStruct(q_t.shape, f32),
            in_specs=[vmem()] * (3 + len(top_dr)), out_specs=vmem(), compiler_params=PARAMS, name="route_grad",
        )(ids_t, q_t, dr.reshape(self.n_ep, -1), *top_dr).T

    def combine(self, q_t, back):
        tok_dev, (n_ep, rows, d), tile = q_t.shape[1], back.shape, 256
        return pl.pallas_call(
            combine_kernel,
            out_shape=jax.ShapeDtypeStruct((tok_dev, d), bf16),
            grid=(tok_dev // tile,),
            in_specs=[pl.BlockSpec((tile, 2), lambda i: (i, 0)), whole((n_ep * rows, d))],
            out_specs=pl.BlockSpec((tile, d), lambda i: (i, 0)),
            compiler_params=PARAMS, name="combine",
        )(q_t.T, back.reshape(n_ep * rows, d))


def solution(mesh):
    n_ep = mesh.shape["ep"]
    tok_spec = P(("fsdp", "ep"), None)
    spec_in = P("ep", "fsdp", None)
    spec_out = P("ep", None, "fsdp")

    def per_device(x_tok, dy_tok, expert_ids, route_w, w_gate, w_up, w_down):
        tok_dev, top_k = expert_ids.shape
        capacity = capacity_of(tok_dev, top_k, w_gate.shape[0] * n_ep)
        part = lax.axis_index("fsdp").astype(i32)
        swap = [(0, 1), (1, 0)]
        own = (w_gate, w_up, w_down)
        weights = [lax.ppermute(w, "fsdp", swap) for w in own]
        ids_t = expert_ids.T
        inputs = (x_tok, dy_tok, ids_t, route_w.T, weights, own)

        def shard_halves(dws):
            out = []
            for dw, axis in zip(dws, (1, 1, 2)):
                size = dw.shape[axis] // 2
                keep = lax.dynamic_slice_in_dim(dw, part * size, size, axis)
                give = lax.dynamic_slice_in_dim(dw, (1 - part) * size, size, axis)
                out.append(keep + lax.ppermute(give, "fsdp", swap))
            return out

        quick = Plan(72, 48, 4, 8, capacity, n_ep, True)
        safe = Plan(2 * capacity, capacity, 1, 1, capacity, n_ep, False)
        notes, top_id, mine, grad_x, grads = quick.forward_top(*inputs)
        agree = jnp.all(notes[:, 1] == top_id.astype(f32)) & jnp.all(notes[:, 0] == 0.0)
        note = jnp.where(agree, top_id.astype(f32), -1.0).reshape(1, 1)
        other = lax.ppermute(note, "fsdp", swap)
        good = agree & (other == note)[0, 0]

        def fits():
            return (grad_x, quick.route_grad(ids_t, *mine), *grads)

        def general():
            q_all, back_all, dr_all, dws = safe.forward(part, *inputs)
            return (safe.combine(q_all, back_all), safe.route_grad(ids_t, q_all, dr_all), *shard_halves(dws))

        return lax.cond(good, fits, general)

    return jax.shard_map(
        per_device, mesh=mesh,
        in_specs=(tok_spec, tok_spec, tok_spec, tok_spec, spec_in, spec_in, spec_out),
        out_specs=(tok_spec, tok_spec, spec_in, spec_in, spec_out),
        check_vma=False)
```
